128 devices in a mesh: lat: 8 (over x, core), lon: 16 (over y, z).
Axes of the slice: x: 4, y: 4, z: 4, core: 2. Of those that a mesh axis runs over, the one named last changes fastest.
Arguments:
- ensemble: bfloat16 [80, 8, 64, 2048], P(None, None, 'lat', 'lon'), may hold values from -6 to 6
- static_sigma: float32 [8], replicated, may hold values from 0.5 to 2
- lat_taps: float32 [17], replicated, may hold values from 0.01 to 0.12
- lon_taps: float32 [17], replicated, may hold values from 0.01 to 0.12
- step_len: float32 [2], replicated, may hold values from 0.2 to 0.6
- send_cols: int32 [8, 16, 128, 64], P('lat', 'lon'), may hold values from 0 to 1023
- send_count: int32 [8, 16, 128], P('lat', 'lon'), may hold values from 32 to 64, as said below
- obs_ref: int32 [8, 16, 4, 2048], P('lat', 'lon'), may hold values from 0 to 8191, as said below
- obs_level: int32 [8, 16, 2048], P('lat', 'lon'), may hold values from 0 to 7
- obs_weight: float32 [8, 16, 4, 2048], P('lat', 'lon'), may hold values from 0 to 1
- innovation: float32 [8, 16, 2048], P('lat', 'lon'), may hold values from -6 to 6
- obs_precision: float32 [8, 16, 2048], P('lat', 'lon'), may hold values from 0.25 to 1
Outputs:
- ens_control: float32 [80, 8, 64, 2048], P(None, None, 'lat', 'lon')
- static_control: float32 [8, 64, 2048], P(None, 'lat', 'lon')
- departures: float32 [8, 16, 2048], P('lat', 'lon')
The draws below stay inside these ranges and needn't reach their ends.
Inputs may be any that keep to these rules, and one draw needn't show every extreme that they name: `send_count`: number of leading slots of send_cols[a, b, e] that are live. One device receives 64 live slots from every device. `obs_ref`: position in the owning device's list L_e of received live columns; always below the total live slots that device receives.
All inputs are finite; a program needn't handle non-finite values.
Results may differ from the reference program's by a relative error of at most 0.0003.
Values may be sent and summed in bfloat16 or wider, within the bound.
No kernel may reach another device: no remote copies, remote signals or barrier semaphores. Data moves between devices by JAX's collectives and lax.ppermute only.
A program may use at most 128 MiB of HBM per device.

```python
import math
import jax
import jax.numpy as jnp
from jax import lax

MEM = 80
LEV = 8
HW = 8
ITERS = 2
CLAT = 8
CLON = 128
NOBS_DEV = 2048
SLOT = 64
NLAT = 64
NLON = 2048
N_LAT = 8
N_LON = 16
DEVICES = 128


def count_table(key):
    table_key = jax.random.fold_in(key, 11)
    lead_key, hot_key = jax.random.split(table_key, 2)
    base_count = jax.random.randint(lead_key, (N_LAT, N_LON, DEVICES), SLOT // 2, SLOT + 1)
    hot_target = jax.random.randint(hot_key, (), 0, DEVICES)
    target = lax.broadcasted_iota(jnp.int32, (N_LAT, N_LON, DEVICES), 2)
    return jnp.where(target == hot_target, SLOT, base_count).astype(jnp.int32)


def draw_send_count(key, part):
    return count_table(key)


def draw_obs_ref(key, part):
    counts = count_table(key).reshape(DEVICES, DEVICES)
    totals = jnp.sum(counts, axis=0).reshape(N_LAT, N_LON, 1, 1)
    raw_draw = jax.random.randint(jax.random.fold_in(key, 23), (N_LAT, N_LON, 4, NOBS_DEV), 0, 2 ** 30)
    return (raw_draw % totals).astype(jnp.int32)


def place_ends(entries, stream_key, low, top_value):
    dims = entries.shape
    index_at = [jax.random.randint(jax.random.fold_in(stream_key, axis), (), 0, dims[axis]) for axis in range(len(dims))]
    entries = entries.at[tuple(index_at)].set(low)
    longest = dims.index(max(dims))
    index_at[longest] = (index_at[longest] + 1) % dims[longest]
    return entries.at[tuple(index_at)].set(top_value)


def shard_levels(stream_key, extent, cuts, smallest, top_value):
    def one(position, blocks):
        draws = jax.random.uniform(jax.random.fold_in(jax.random.fold_in(stream_key, 6), position), (blocks,), jnp.float32, smallest / len(cuts), top_value / len(cuts))
        return jnp.repeat(jnp.exp(draws), extent[position] // blocks).reshape((-1,) + (1,) * (len(extent) - position - 1))

    factor_of = one(*cuts[0])
    for cut in cuts[1:]:
        factor_of = factor_of * one(*cut)
    return factor_of


def scatter_about(stream_key, shape, width, bound, cuts=(), kind=jnp.bfloat16):
    values = width * jax.random.normal(stream_key, shape, jnp.float32)
    if cuts:
        values = values * shard_levels(stream_key, shape, cuts, -0.22, 0.18)
    return jnp.clip(values, -bound, bound).astype(kind)


def setup_inputs(seed: int = 0) -> dict:
    streams_of = jax.random.split(jax.random.key(seed), 13)
    ensemble = scatter_about(streams_of[0], (MEM, LEV, NLAT, NLON), 1.0, 6.0, ((2, 8), (3, 16)))
    static_sigma = jnp.clip(jnp.exp(jax.random.uniform(streams_of[1], (LEV,), jnp.float32, math.log(0.5), math.log(2.0))), 0.5, 2.0)
    lat_taps = jnp.clip(jnp.exp(jax.random.uniform(streams_of[2], (2 * HW + 1,), jnp.float32, math.log(0.01), math.log(0.12))), 0.01, 0.12)
    lon_taps = jnp.clip(jnp.exp(jax.random.uniform(streams_of[3], (2 * HW + 1,), jnp.float32, math.log(0.01), math.log(0.12))), 0.01, 0.12)
    step_len = jnp.clip(jax.random.uniform(streams_of[4], (ITERS,), jnp.float32, 0.2, 0.6), 0.2, 0.6)
    send_cols = place_ends(jax.random.randint(streams_of[5], (N_LAT, N_LON, DEVICES, SLOT), 0, CLAT * CLON), jax.random.fold_in(streams_of[5], 1), 0, (CLAT * CLON) - 1).astype(jnp.int32)
    send_count = draw_send_count(jax.random.fold_in(streams_of[12], 71), 0)
    obs_ref = draw_obs_ref(jax.random.fold_in(streams_of[12], 71), 0)
    obs_level = place_ends(jax.random.randint(streams_of[8], (N_LAT, N_LON, NOBS_DEV), 0, LEV), jax.random.fold_in(streams_of[8], 1), 0, LEV - 1).astype(jnp.int32)
    obs_weight = jnp.clip(1.0 * jax.random.uniform(streams_of[9], (N_LAT, N_LON, 4, NOBS_DEV), jnp.float32) ** shard_levels(streams_of[9], (N_LAT, N_LON, 4, NOBS_DEV), ((0, 8), (1, 16)), -0.2, 0.2), 0.0, 1.0)
    innovation = scatter_about(streams_of[10], (N_LAT, N_LON, NOBS_DEV), 1.0, 6.0, ((0, 8), (1, 16)), jnp.float32)
    obs_precision = jnp.clip(jnp.exp(math.log(1.0) - 1.3862944 * jax.random.uniform(streams_of[11], (N_LAT, N_LON, NOBS_DEV), jnp.float32) ** shard_levels(streams_of[11], (N_LAT, N_LON, NOBS_DEV), ((0, 8), (1, 16)), -0.2, 0.2)), 0.25, 1.0)
    return dict(ensemble=ensemble, static_sigma=static_sigma, lat_taps=lat_taps, lon_taps=lon_taps, step_len=step_len, send_cols=send_cols, send_count=send_count, obs_ref=obs_ref, obs_level=obs_level, obs_weight=obs_weight, innovation=innovation, obs_precision=obs_precision)


HYBRID_STATIC = 0.5
HYBRID_ENSEMBLE = 0.8660254037844386

def smooth_whole(fields, lat_taps, lon_taps):
    half_width = (lat_taps.shape[0] - 1) // 2
    lat_count = fields.shape[1]
    padded = jnp.pad(fields, ((0, 0), (half_width, half_width), (0, 0)))
    lat_pass = jnp.zeros_like(fields)
    for offset in range(2 * half_width + 1):
        lat_pass = lat_pass + lat_taps[offset] * padded[:, offset:offset + lat_count, :]
    result = jnp.zeros_like(fields)
    for offset in range(2 * half_width + 1):
        result = result + lon_taps[offset] * jnp.roll(lat_pass, half_width - offset, axis=2)
    return result

def smooth_adjoint(fields, lat_taps, lon_taps):
    half_width = (lat_taps.shape[0] - 1) // 2
    lat_count = fields.shape[1]
    lat_flip = lat_taps[::-1]
    lon_flip = lon_taps[::-1]
    lon_pass = jnp.zeros_like(fields)
    for offset in range(2 * half_width + 1):
        lon_pass = lon_pass + lon_flip[offset] * jnp.roll(fields, half_width - offset, axis=2)
    padded = jnp.pad(lon_pass, ((0, 0), (half_width, half_width), (0, 0)))
    result = jnp.zeros_like(fields)
    for offset in range(2 * half_width + 1):
        result = result + lat_flip[offset] * padded[:, offset:offset + lat_count, :]
    return result

def reference(ensemble, static_sigma, lat_taps, lon_taps, step_len, send_cols, send_count, obs_ref, obs_level, obs_weight, innovation, obs_precision):
    device_count = N_LAT * N_LON
    slot_count = send_cols.shape[-1]
    members, level_count, lat_total, lon_total = ensemble.shape
    lat_rows = lat_total // N_LAT
    lon_cells = lon_total // N_LON
    counts = send_count.reshape(device_count, device_count)
    slot_ends = jnp.cumsum(counts, axis=0)
    column_table = send_cols.reshape(device_count, device_count, slot_count)
    positions = obs_ref.reshape(device_count, 4, -1)

    def locate(target):
        target_ends = slot_ends[:, target]
        source = jnp.searchsorted(target_ends, positions[target], side='right').astype(jnp.int32)
        first_slot = (target_ends - counts[:, target])[source]
        local_cell = column_table[source, target, positions[target] - first_slot]
        grid_row = source // N_LON * lat_rows + local_cell // lon_cells
        grid_col = source % N_LON * lon_cells + local_cell % lon_cells
        return (grid_row, grid_col)
    grid_rows, grid_cols = jax.vmap(locate)(jnp.arange(device_count, dtype=jnp.int32))
    levels = jnp.broadcast_to(obs_level.reshape(device_count, 1, -1), grid_rows.shape)
    weights = obs_weight.reshape(device_count, 4, -1)
    innovations = innovation.reshape(device_count, -1)
    precision_obs = obs_precision.reshape(device_count, -1)
    ens_scale = HYBRID_ENSEMBLE / math.sqrt(members - 1)
    sigma = static_sigma[:, None, None]
    control = jnp.zeros(ensemble.shape, jnp.float32)
    static = jnp.zeros((level_count, lat_total, lon_total), jnp.float32)
    departure = -innovations
    for iteration in range(ITERS):
        if iteration > 0:

            def accumulate(running, member_pair):
                member, member_control = member_pair
                return (running + member.astype(jnp.float32) * smooth_whole(member_control, lat_taps, lon_taps), None)
            ens_part, unused = lax.scan(accumulate, jnp.zeros((level_count, lat_total, lon_total), jnp.float32), (ensemble, control))
            increment = ens_scale * ens_part + HYBRID_STATIC * sigma * smooth_whole(static, lat_taps, lon_taps)
            departure = lax.optimization_barrier(jnp.sum(weights * increment[levels, grid_rows, grid_cols], axis=1)) - innovations
        forcing = jnp.zeros((level_count, lat_total, lon_total), jnp.float32).at[levels, grid_rows, grid_cols].add(weights * (precision_obs * departure)[:, None, :])
        adjoint = lax.map(lambda member: smooth_adjoint(member.astype(jnp.float32) * forcing, lat_taps, lon_taps), ensemble)
        control = control - step_len[iteration] * (ens_scale * adjoint + control)
        static = static - step_len[iteration] * (HYBRID_STATIC * sigma * smooth_adjoint(forcing, lat_taps, lon_taps) + static)
    return (control, static, departure.reshape(N_LAT, N_LON, -1))
```

```python
import functools
import math

import jax
import jax.numpy as jnp
from jax import lax
from jax.experimental import pallas as pl
from jax.experimental.pallas import tpu as pltpu
from jax.sharding import PartitionSpec as P

HYBRID_STATIC = 0.5
HYBRID_ENSEMBLE = 0.8660254037844386
F32 = jnp.float32
BF16 = jnp.bfloat16
I32 = jnp.int32

MEM = 80
LEV = 8
ROWS = 8
LANES = 128
NOBS = 2048
SLOT = 64
DEV = 128
NLAT = 64
HW = 8
TAPS = 17
EDGE = 16
BUF = DEV * 4

VMEM = pltpu.VMEM
ARB = ("arbitrary",)


def whole(memory_space=VMEM):
    return pl.BlockSpec(memory_space=memory_space)


def split(value):
    high = value.astype(BF16).astype(F32)
    return high, value - high


def iota(shape, dim):
    return lax.broadcasted_iota(I32, shape, dim)


def nn(a, b):
    return lax.dot_general(a, b, (((1,), (0,)), ((), ())), preferred_element_type=F32)


def nt(a, b):
    return lax.dot_general(a, b, (((1,), (1,)), ((), ())), preferred_element_type=F32)


def matrices_kernel(band_ref, lat_ref, lon_ref, lat_mid, lon_mid, lat_fin, lon_fin):
    base = band_ref[0] * ROWS

    def pick(index, taps):
        out = jnp.zeros(index.shape, F32)
        for t in range(TAPS):
            out = jnp.where(index == t, taps[t], out)
        return out

    row = iota((8, 160), 0)
    col = iota((8, 160), 1)
    group = sum((col >= 40 * n).astype(I32) for n in range(1, 4))
    offset = col - 40 * group
    diff = row - offset + 2 * HW
    source = base - 2 * HW + offset
    total = jnp.zeros((8, 160), F32)
    for t in range(TAPS):
        middle = base + row + t - HW
        valid = jnp.logical_and(middle >= 0, middle < NLAT)
        total = total + jnp.where(valid, lat_ref[t] * pick(diff + t, lat_ref), 0.0)
    total = jnp.where(jnp.logical_and(source >= 0, source < NLAT), total, 0.0)
    high, low = split(total)
    blocks = []
    for s in range(2):
        blocks.append(jnp.where((group >> 1) == s, high, 0.0))
        blocks.append(jnp.where(group == 2 * s, low, 0.0))
    lat_mid[...] = jnp.concatenate(blocks, axis=0).astype(BF16)

    row = iota((8, 192), 0)
    col = iota((8, 192), 1)
    group = sum((col >= 24 * n).astype(I32) for n in range(1, 8))
    offset = col - 24 * group
    source = base - HW + offset
    total = pick(row - offset + 2 * HW, lat_ref)
    total = jnp.where(jnp.logical_and(source >= 0, source < NLAT), total, 0.0)
    high, low = split(total)
    blocks = []
    for s in range(4):
        blocks.append(jnp.where((group >> 1) == s, high, 0.0))
        blocks.append(jnp.where(group == 2 * s, low, 0.0))
    lat_fin[...] = jnp.concatenate(blocks, axis=0).astype(BF16)

    lag = iota((8, LANES), 1) - 2 * HW
    auto = jnp.zeros((8, LANES), F32)
    for t in range(TAPS):
        auto = auto + lon_ref[t] * pick(lag + t, lon_ref)

    def auto_at(n):
        return jnp.sum(jnp.where(lag[:1] == n, auto[:1], 0.0), axis=1, keepdims=True)

    coefficients = [auto_at(n) for n in range(2 * HW + 1)]
    main = iota((LANES, LANES), 0) - iota((LANES, LANES), 1)
    edge = iota((32, LANES), 0)
    edge = jnp.where(edge < EDGE, edge - EDGE, edge + LANES - EDGE) - iota((32, LANES), 1)

    def smooth_twice(distance):
        distance = jnp.abs(distance)
        out = jnp.zeros(distance.shape, F32)
        for n in range(2 * HW + 1):
            out = jnp.where(distance == n, coefficients[n], out)
        return out

    def place(out_ref, main_value, edge_value):
        main_high, main_low = split(main_value)
        edge_high, edge_low = split(edge_value)
        for v in range(4):
            out_ref[v, :LANES, :LANES] = main_high.astype(BF16)
            out_ref[v, :LANES, LANES:] = main_low.astype(BF16)
            out_ref[v, LANES:, :] = jnp.zeros((LANES, 2 * LANES), BF16)
            out_ref[v, LANES + 32 * v : LANES + 32 * (v + 1), :LANES] = edge_high.astype(BF16)
            out_ref[v, LANES + 32 * v : LANES + 32 * (v + 1), LANES:] = edge_low.astype(BF16)

    place(lon_mid, smooth_twice(main), smooth_twice(edge))
    place(lon_fin, pick(HW - main, lon_ref), pick(HW - edge, lon_ref))


def matrices(band, lat_taps, lon_taps):
    smem = whole(pltpu.SMEM)
    return pl.pallas_call(
        matrices_kernel,
        out_shape=(
            jax.ShapeDtypeStruct((32, 160), BF16),
            jax.ShapeDtypeStruct((4, 256, 256), BF16),
            jax.ShapeDtypeStruct((64, 192), BF16),
            jax.ShapeDtypeStruct((4, 256, 256), BF16),
        ),
        in_specs=[smem] * 3,
        out_specs=(whole(),) * 4,
        cost_estimate=pl.CostEstimate(flops=4000000, bytes_accessed=1100000, transcendentals=0),
        name="matrices",
    )(band, lat_taps, lon_taps)


def pack_kernel(e_ref, out_ref):
    row = iota((LANES, LANES), 0)
    col = iota((LANES, LANES), 1)
    inner = col & 31
    source = jnp.where(inner < EDGE, inner + LANES - EDGE, inner - EDGE)
    count = e_ref.shape[0]
    for g in range(2):
        total = None
        for v in range(4):
            choose = jnp.logical_and(row == source, (col >> 5) == v)
            choose = jnp.where(choose, 1.0, 0.0).astype(BF16)
            tile = e_ref[:, 4 * g + v].astype(F32).reshape(count * ROWS, LANES).astype(BF16)
            part = nn(tile, choose)
            total = part if total is None else total + part
        out_ref[:, g] = total.reshape(count, ROWS, LANES).astype(BF16)


def pack(ensemble):
    step = 16
    return pl.pallas_call(
        pack_kernel,
        grid=(MEM // step,),
        out_shape=jax.ShapeDtypeStruct((MEM, 2, ROWS, LANES), BF16),
        in_specs=[pl.BlockSpec((step, LEV, ROWS, LANES), lambda i: (i, 0, 0, 0))],
        out_specs=pl.BlockSpec((step, 2, ROWS, LANES), lambda i: (i, 0, 0, 0)),
        compiler_params=pltpu.CompilerParams(dimension_semantics=ARB),
        cost_estimate=pl.CostEstimate(flops=4000000, bytes_accessed=1600000, transcendentals=0),
        name="pack",
    )(ensemble)


CHUNK = 256


def place_values(acc_ref, row_hot, lane_of, value_of, lane_iota):
    parts_high, parts_low = [], []
    for q in range(4):
        hit = lane_iota == lane_of[q]
        high, low = split(value_of[q])
        parts_high.append(jnp.where(hit, high, 0.0).astype(BF16))
        parts_low.append(jnp.where(hit, low, 0.0).astype(BF16))
    values = jnp.concatenate(
        [jnp.concatenate(parts_high, axis=1), jnp.concatenate(parts_low, axis=1)], axis=0
    )
    acc_ref[...] += nt(row_hot, values)


def hot_rows(row_of, row_iota):
    parts = [jnp.where(row_iota == row_of[q], 1.0, 0.0).astype(BF16) for q in range(4)]
    return jnp.concatenate(parts, axis=1)


def first_kernel(
    count_ref, ref_ref, level_ref, weight_ref, precision_ref, innovation_ref,
    buffer_ref, row_ref, lane_ref, acc_ref,
):
    count = count_ref[...].astype(F32)
    sub = iota((DEV, DEV), 0)
    lane = iota((DEV, DEV), 1)
    ends = jnp.sum(jnp.where(lane <= sub, count, 0.0), axis=1, keepdims=True)
    counts = jnp.sum(jnp.where(lane == sub, count, 0.0), axis=1, keepdims=True)
    acc_ref[...] = jnp.zeros_like(acc_ref)
    row_iota = iota((BUF, CHUNK), 0).astype(F32)
    lane_iota = iota((LANES, CHUNK), 0).astype(F32)

    @pl.loop(0, NOBS // CHUNK)
    def _(c):
        part = pl.ds(pl.multiple_of(c * CHUNK, CHUNK), CHUNK)
        level = level_ref[:, part]
        low_level = (level & 3).astype(F32)
        high_level = ((level >> 2) * SLOT).astype(F32)
        forced = -(precision_ref[:, part] * innovation_ref[:, part])
        rows, lanes, values = [], [], []
        for q in range(4):
            position = ref_ref[q : q + 1, part].astype(F32)
            passed = position >= ends
            source = jnp.sum(jnp.where(passed, 1.0, 0.0), axis=0, keepdims=True)
            start = jnp.sum(jnp.where(passed, counts, 0.0), axis=0, keepdims=True)
            rows.append(source * 4.0 + low_level)
            lanes.append(high_level + position - start)
            row_ref[q : q + 1, part] = rows[q]
            lane_ref[q : q + 1, part] = lanes[q]
            values.append(weight_ref[q : q + 1, part] * forced)
        place_values(acc_ref, hot_rows(rows, row_iota), lanes, values, lane_iota)

    buffer_ref[...] = acc_ref[:, :LANES] + acc_ref[:, LANES:]


def first(count, ref, level, weight, precision, innovation):
    return pl.pallas_call(
        first_kernel,
        out_shape=(
            jax.ShapeDtypeStruct((BUF, LANES), F32),
            jax.ShapeDtypeStruct((4, NOBS), F32),
            jax.ShapeDtypeStruct((4, NOBS), F32),
        ),
        in_specs=[whole()] * 6,
        out_specs=(whole(),) * 3,
        scratch_shapes=[VMEM((BUF, 2 * LANES), F32)],
        cost_estimate=pl.CostEstimate(flops=40000000, bytes_accessed=600000, transcendentals=0),
        name="first",
    )(count, ref, level, weight, precision, innovation)


def second_kernel(
    incoming_ref, row_ref, lane_ref, weight_ref, precision_ref, innovation_ref, coef_ref,
    buffer_ref, departure_ref, acc_ref,
):
    flipped = incoming_ref[...].T
    high, low = split(flipped)
    table = jnp.concatenate([high, low], axis=0).astype(BF16)
    acc_ref[...] = jnp.zeros_like(acc_ref)
    row_iota = iota((BUF, CHUNK), 0).astype(F32)
    lane_iota = iota((LANES, CHUNK), 0).astype(F32)
    earlier = coef_ref[3, :1, :1]
    later = coef_ref[4, :1, :1]

    @pl.loop(0, NOBS // CHUNK)
    def _(c):
        part = pl.ds(pl.multiple_of(c * CHUNK, CHUNK), CHUNK)
        rows = [row_ref[q : q + 1, part] for q in range(4)]
        lanes = [lane_ref[q : q + 1, part] for q in range(4)]
        weights = [weight_ref[q : q + 1, part] for q in range(4)]
        innovation = innovation_ref[:, part]
        row_hot = hot_rows(rows, row_iota)
        found = nn(table, row_hot)
        found = found[:LANES] + found[LANES:]
        departure = -innovation
        for q in range(4):
            column = found[:, q * CHUNK : (q + 1) * CHUNK]
            picked = jnp.sum(jnp.where(lane_iota == lanes[q], column, 0.0), axis=0, keepdims=True)
            departure = departure + weights[q] * picked
        departure_ref[:, part] = departure
        forced = precision_ref[:, part] * (later * departure - earlier * innovation)
        values = [weights[q] * forced for q in range(4)]
        place_values(acc_ref, row_hot, lanes, values, lane_iota)

    buffer_ref[...] = acc_ref[:, :LANES] + acc_ref[:, LANES:]


def second(incoming, rows, lanes, weight, precision, innovation, coefs):
    return pl.pallas_call(
        second_kernel,
        out_shape=(
            jax.ShapeDtypeStruct((BUF, LANES), F32),
            jax.ShapeDtypeStruct((1, NOBS), F32),
        ),
        in_specs=[whole()] * 7,
        out_specs=(whole(),) * 2,
        scratch_shapes=[VMEM((BUF, 2 * LANES), F32)],
        cost_estimate=pl.CostEstimate(flops=60000000, bytes_accessed=800000, transcendentals=0),
        name="second",
    )(incoming, rows, lanes, weight, precision, innovation, coefs)


def swap_quadrants(tile):
    sub = iota((8, LANES), 0) < 4
    lane = iota((8, LANES), 1) < SLOT
    moved = pltpu.roll(pltpu.roll(tile, 4, 0), SLOT, 1)
    return jnp.where(sub == lane, tile, moved)


PAIRS = DEV // 2
GROUP = 4


def columns_kernel(buffer_ref, cell_ref, out_ref, acc_ref, grid_ref):
    acc_ref[...] = jnp.zeros_like(acc_ref)
    lane_iota = iota((LANES, LANES), 0)

    @pl.loop(0, PAIRS // GROUP)
    def _(n):
        values, hots = [], []
        for g in range(GROUP):
            m = n * GROUP + g
            tile = swap_quadrants(buffer_ref[pl.ds(pl.multiple_of(m * 8, 8), 8), :])
            cell = cell_ref[pl.ds(m, 1), :]
            row = cell >> 7
            high, low = split(tile)
            masks = [row == r for r in range(ROWS)]
            values.append(
                jnp.concatenate(
                    [jnp.where(k, high, 0.0) for k in masks] + [jnp.where(k, low, 0.0) for k in masks],
                    axis=0,
                ).astype(BF16)
            )
            hots.append(jnp.where(lane_iota == (cell & 127), 1.0, 0.0).astype(BF16))
        acc_ref[...] += nt(jnp.concatenate(values, axis=1), jnp.concatenate(hots, axis=1))

    grid_ref[...] = acc_ref[:64] + acc_ref[64:]
    lane = iota((ROWS, LANES), 1)
    inner = lane & 31
    edges = [jnp.zeros((ROWS, LANES), F32)] * 2
    for l in range(LEV):
        tile = grid_ref[pl.ds(l, ROWS, stride=LEV), :]
        out_ref[l] = tile
        v = l % 4
        right = pltpu.roll(tile, (32 * v + EDGE) % LANES, 1)
        left = pltpu.roll(tile, (32 * v + EDGE) % LANES, 1)
        moved = jnp.where(inner < EDGE, right, left)
        edges[l // 4] = jnp.where((lane >> 5) == v, moved, edges[l // 4])
    out_ref[LEV] = edges[0]
    out_ref[LEV + 1] = edges[1]


def columns(buffer, cells):
    return pl.pallas_call(
        columns_kernel,
        out_shape=jax.ShapeDtypeStruct((LEV + 2, ROWS, LANES), F32),
        in_specs=[whole()] * 2,
        out_specs=whole(),
        scratch_shapes=[VMEM((LANES, LANES), F32), VMEM((64, LANES), F32)],
        cost_estimate=pl.CostEstimate(flops=20000000, bytes_accessed=400000, transcendentals=0),
        name="columns",
    )(buffer, cells)


def slots_kernel(increment_ref, cell_ref, out_ref):
    rows = [increment_ref[pl.ds(r, LEV, stride=ROWS), :] for r in range(ROWS)]
    pairs = [split(value) for value in rows]
    table = jnp.concatenate([p[0] for p in pairs] + [p[1] for p in pairs], axis=0).astype(BF16)
    lane_iota = iota((LANES, LANES), 0)

    @pl.loop(0, PAIRS // GROUP)
    def _(n):
        hots, cells = [], []
        for g in range(GROUP):
            cell = cell_ref[pl.ds(n * GROUP + g, 1), :]
            cells.append(cell >> 7)
            hots.append(jnp.where(lane_iota == (cell & 127), 1.0, 0.0).astype(BF16))
        found = nn(table, jnp.concatenate(hots, axis=1))
        found = found[:64] + found[64:]
        for g in range(GROUP):
            tile = jnp.zeros((LEV, LANES), F32)
            for r in range(ROWS):
                part = found[8 * r : 8 * r + 8, g * LANES : (g + 1) * LANES]
                tile = jnp.where(cells[g] == r, part, tile)
            m = n * GROUP + g
            out_ref[pl.ds(pl.multiple_of(m * 8, 8), 8), :] = swap_quadrants(tile)


def slots(increment, cells):
    return pl.pallas_call(
        slots_kernel,
        out_shape=jax.ShapeDtypeStruct((BUF, LANES), F32),
        in_specs=[whole()] * 2,
        out_specs=whole(),
        cost_estimate=pl.CostEstimate(flops=20000000, bytes_accessed=400000, transcendentals=0),
        name="slots",
    )(increment, cells)


def row_pass(e_refs, fields, lat_ref, stack, prod_ref, out_ref, lane0):
    per = MEM // stack
    height = 2 * ROWS * len(fields)

    def column_of(tiles):
        highs, lows = zip(*[split(t) for t in tiles])
        return jnp.concatenate(list(highs) + list(lows), axis=0).astype(BF16)

    @pl.loop(0, per)
    def _(n):
        for s in range(stack):
            tiles = [e[s * per + n, 0].astype(F32) * f for e, f in zip(e_refs, fields)]
            prod_ref[s * height : (s + 1) * height, pl.ds(pl.multiple_of(n * LANES, LANES), LANES)] = (
                column_of(tiles)
            )

    prod_ref[:, per * LANES :] = jnp.zeros((stack * height, LANES), BF16)
    prod_ref[:height, per * LANES :] = column_of(fields)
    lat = lat_ref[...]

    def store(row, value):
        high, low = split(value)
        out_ref[0, pl.ds(row, 16), lane0 : lane0 + LANES] = high.astype(BF16)
        out_ref[1, pl.ds(row, 16), lane0 : lane0 + LANES] = low.astype(BF16)

    def block(value, s, n):
        tile = value[16 * s : 16 * s + 16, n * LANES : (n + 1) * LANES]
        return tile[:8] + tile[8:]

    wide = 4

    @pl.loop(0, per // wide)
    def _(c):
        start = pl.multiple_of(c * (wide * LANES), wide * LANES)
        value = nn(lat, prod_ref[:, pl.ds(start, wide * LANES)])
        for s in range(stack):
            for n in range(0, wide, 2):
                pair = jnp.concatenate([block(value, s, n), block(value, s, n + 1)], axis=0)
                store(pl.multiple_of((s * per + c * wide + n) * 8, 16), pair)

    value = nn(lat, prod_ref[:, per * LANES :])
    one = block(value, 0, 0)
    store(MEM * 8, jnp.concatenate([one, jnp.zeros_like(one)], axis=0))


def column_pass(in_ref, weights, start, size):
    value = nn(in_ref[0, pl.ds(start, size), :], weights)
    value = value + nn(in_ref[1, pl.ds(start, size), :], weights)
    return value[:, :LANES] + value[:, LANES:]


def merge_edges(left, right):
    inner = iota((ROWS, LANES), 1) & 31
    return jnp.where(inner < EDGE, left, right)


BLOCKS = 5


def middle_kernel(*refs):
    e_refs = refs[:5]
    h_refs = refs[5:10]
    f_refs = refs[10:15]
    left_ref, right_ref, lat_ref, lon_ref, coef_ref, out_ref, prod_ref, pass_ref = refs[15:]
    l = pl.program_id(0)

    @pl.when((l & 3) == 0)
    def _():
        g = l >> 2
        fields = [merge_edges(left_ref[x, g], right_ref[x, g]) for x in range(5)]
        row_pass(h_refs, fields, lat_ref, 2, prod_ref, pass_ref, LANES)

    fields = [f_refs[x][l] for x in range(5)]
    row_pass(e_refs, fields, lat_ref, 2, prod_ref, pass_ref, 0)
    weights = lon_ref[0]
    step = 16

    def part(c, total):
        value = column_pass(pass_ref, weights, pl.multiple_of(c * (8 * step), 8 * step), 8 * step)
        own = e_refs[2][pl.ds(c * step, step), 0].astype(F32)
        return total + jnp.sum(value.reshape(step, ROWS, LANES) * own, axis=0)

    total = lax.fori_loop(0, MEM // step, part, jnp.zeros((ROWS, LANES), F32))
    single = column_pass(pass_ref, weights, MEM * 8, 16)[:8]
    out_ref[0] = coef_ref[0] * total + coef_ref[1, pl.ds(l, 1), :] * single


def level_block(count):
    return pl.BlockSpec((count, 1, ROWS, LANES), lambda l: (0, l, 0, 0))


def edge_block(count):
    return pl.BlockSpec((count, 1, ROWS, LANES), lambda l: (0, l // 4, 0, 0))


def middle(members, halos, fields, left, right, lat_mid, lon_mid, coefs):
    return pl.pallas_call(
        middle_kernel,
        grid=(LEV,),
        out_shape=jax.ShapeDtypeStruct((LEV, ROWS, LANES), F32),
        in_specs=[level_block(MEM)] * 5
        + [edge_block(MEM)] * 5
        + [whole()] * 8
        + [pl.BlockSpec((1, 256, 256), lambda l: (l % 4, 0, 0)), whole()],
        out_specs=pl.BlockSpec((1, ROWS, LANES), lambda l: (l, 0, 0)),
        scratch_shapes=[VMEM((160, 41 * LANES), BF16), VMEM((2, MEM * 8 + 16, 256), BF16)],
        compiler_params=pltpu.CompilerParams(dimension_semantics=ARB),
        cost_estimate=pl.CostEstimate(flops=100000000, bytes_accessed=9000000, transcendentals=0),
        name="middle",
    )(*members, *halos, *fields, left, right, lat_mid, lon_mid, coefs)


def final_kernel(*refs):
    e_refs = refs[:3]
    h_refs = refs[3:6]
    f_refs = refs[6:9]
    left_ref, right_ref, lat_ref, lon_ref, coef_ref, out_ref, static_ref, prod_ref, pass_ref = refs[9:]
    l = pl.program_id(0)

    @pl.when((l & 3) == 0)
    def _():
        g = l >> 2
        fields = [merge_edges(left_ref[x, g], right_ref[x, g]) for x in range(3)]
        row_pass(h_refs, fields, lat_ref, 4, prod_ref, pass_ref, LANES)

    fields = [f_refs[x][l] for x in range(3)]
    row_pass(e_refs, fields, lat_ref, 4, prod_ref, pass_ref, 0)
    weights = lon_ref[0]
    step = 16
    scale = -HYBRID_ENSEMBLE / math.sqrt(MEM - 1)

    @pl.loop(0, MEM // step)
    def _(c):
        value = column_pass(pass_ref, weights, pl.multiple_of(c * (8 * step), 8 * step), 8 * step)
        out_ref[pl.ds(c * step, step), 0] = (scale * value).reshape(step, ROWS, LANES)

    single = column_pass(pass_ref, weights, MEM * 8, 16)[:8]
    static_ref[0] = coef_ref[2, pl.ds(l, 1), :] * single


def final(members, halos, fields, left, right, lat_fin, lon_fin, coefs):
    return pl.pallas_call(
        final_kernel,
        grid=(LEV,),
        out_shape=(
            jax.ShapeDtypeStruct((MEM, LEV, ROWS, LANES), F32),
            jax.ShapeDtypeStruct((LEV, ROWS, LANES), F32),
        ),
        in_specs=[level_block(MEM)] * 3
        + [edge_block(MEM)] * 3
        + [whole()] * 6
        + [pl.BlockSpec((1, 256, 256), lambda l: (l % 4, 0, 0)), whole()],
        out_specs=(level_block(MEM), pl.BlockSpec((1, ROWS, LANES), lambda l: (l, 0, 0))),
        scratch_shapes=[VMEM((192, 21 * LANES), BF16), VMEM((2, MEM * 8 + 16, 256), BF16)],
        compiler_params=pltpu.CompilerParams(dimension_semantics=ARB),
        cost_estimate=pl.CostEstimate(flops=100000000, bytes_accessed=9000000, transcendentals=0),
        name="final",
    )(*members, *halos, *fields, left, right, lat_fin, lon_fin, coefs)


def shift(value, axis, step):
    count = lax.axis_size(axis)
    return lax.ppermute(value, axis, [(i, (i + step) % count) for i in range(count)])


def route(buffer):
    buffer = buffer.reshape(DEV, 4, LANES)
    out = lax.all_to_all(buffer, ("lat", "lon"), split_axis=0, concat_axis=0, tiled=True)
    return out.reshape(BUF, LANES)


def per_device(
    ensemble,
    static_sigma,
    lat_taps,
    lon_taps,
    step_len,
    send_cols,
    send_count,
    obs_ref,
    obs_level,
    obs_weight,
    innovation,
    obs_precision,
):
    ens_scale = HYBRID_ENSEMBLE / math.sqrt(MEM - 1)
    received = lax.all_to_all(
        send_count, ("lat", "lon"), split_axis=2, concat_axis=2, tiled=True
    ).reshape(1, DEV)
    cells = send_cols.reshape(PAIRS, LANES)
    level = obs_level.reshape(1, NOBS)
    ref = obs_ref.reshape(4, NOBS)
    weight = obs_weight.reshape(4, NOBS)
    innov = innovation.reshape(1, NOBS)
    precision = obs_precision.reshape(1, NOBS)

    ones = jnp.ones((LEV, LANES), F32)
    sigma = static_sigma[:, None] * ones
    coefs = jnp.stack(
        [
            (-step_len[0] * ens_scale * ens_scale) * ones,
            (-step_len[0] * HYBRID_STATIC * HYBRID_STATIC) * sigma * sigma,
            -HYBRID_STATIC * sigma,
            ((1.0 - step_len[1]) * step_len[0]) * ones,
            step_len[1] * ones,
        ]
    )
    band = lax.axis_index("lat").astype(I32).reshape(1)
    lat_mid, lon_mid, lat_fin, lon_fin = matrices(band, lat_taps, lon_taps)

    packed = pack(ensemble)
    from_left = shift(packed, "lon", 1)
    from_right = shift(packed, "lon", -1)
    inner = lax.broadcasted_iota(I32, packed.shape, 3) & 31
    halo = jnp.where(inner < EDGE, from_left, from_right)
    north = shift(ensemble, "lat", 1)
    south = shift(ensemble, "lat", -1)
    north2 = shift(north, "lat", 1)
    south2 = shift(south, "lat", -1)
    halo_n = shift(halo, "lat", 1)
    halo_s = shift(halo, "lat", -1)
    halo_n2 = shift(halo_n, "lat", 1)
    halo_s2 = shift(halo_s, "lat", -1)

    outgoing, rows, lanes = first(received, ref, level, weight, precision, innov)
    forcing = columns(route(outgoing), cells)
    fields = [
        shift(forcing, "lat", 2),
        shift(forcing, "lat", 1),
        forcing,
        shift(forcing, "lat", -1),
        shift(forcing, "lat", -2),
    ]
    edges = jnp.stack([f[LEV:] for f in fields])
    increment = middle(
        (north2, north, ensemble, south, south2),
        (halo_n2, halo_n, halo, halo_s, halo_s2),
        fields,
        shift(edges, "lon", 1),
        shift(edges, "lon", -1),
        lat_mid,
        lon_mid,
        coefs,
    )
    incoming = route(slots(increment.reshape(LEV * ROWS, LANES), cells))
    outgoing, departure = second(incoming, rows, lanes, weight, precision, innov, coefs)
    forcing = columns(route(outgoing), cells)
    fields = [shift(forcing, "lat", 1), forcing, shift(forcing, "lat", -1)]
    edges = jnp.stack([f[LEV:] for f in fields])
    control, static = final(
        (north, ensemble, south),
        (halo_n, halo, halo_s),
        fields,
        shift(edges, "lon", 1),
        shift(edges, "lon", -1),
        lat_fin,
        lon_fin,
        coefs,
    )
    return (control, static, departure.reshape(1, 1, -1))


def solution(mesh):
    return jax.shard_map(
        per_device,
        mesh=mesh,
        in_specs=(
            P(None, None, "lat", "lon"),
            P(),
            P(),
            P(),
            P(),
            P("lat", "lon", None, None),
            P("lat", "lon", None),
            P("lat", "lon", None, None),
            P("lat", "lon", None),
            P("lat", "lon", None, None),
            P("lat", "lon", None),
            P("lat", "lon", None),
        ),
        out_specs=(P(None, None, "lat", "lon"), P(None, "lat", "lon"), P("lat", "lon", None)),
        check_vma=False,
    )
```

```python
import math

import jax
import jax.numpy as jnp
from jax import lax
from jax.experimental import pallas as pl
from jax.experimental.pallas import tpu as pltpu
from jax.sharding import PartitionSpec as P


HYBRID_STATIC = 0.5
HYBRID_ENSEMBLE = 0.8660254037844386
F32 = jnp.float32
BF16 = jnp.bfloat16
I32 = jnp.int32

MEM = 80
LEV = 8
ROWS = 8
LANES = 128
NOBS = 2048
SLOT = 64
DEV = 128
NLAT = 64
HW = 8
TAPS = 17
EDGE = 16
BUF = DEV * 4

VMEM = pltpu.VMEM
ARB = ("arbitrary",)


def whole(memory_space=VMEM):
    return pl.BlockSpec(memory_space=memory_space)


def split(value):
    high = value.astype(BF16).astype(F32)
    return high, value - high


def iota(shape, dim):
    return lax.broadcasted_iota(I32, shape, dim)


def nn(a, b):
    return lax.dot_general(a, b, (((1,), (0,)), ((), ())), preferred_element_type=F32)


def nt(a, b):
    return lax.dot_general(a, b, (((1,), (1,)), ((), ())), preferred_element_type=F32)


def matrices_kernel(band_ref, lat_ref, lon_ref, lat_mid, lon_mid, lat_fin, lon_fin):
    base = band_ref[0] * ROWS

    def pick(index, taps):
        out = jnp.zeros(index.shape, F32)
        for t in range(TAPS):
            out = jnp.where(index == t, taps[t], out)
        return out

    row = iota((8, 160), 0)
    col = iota((8, 160), 1)
    group = sum((col >= 40 * n).astype(I32) for n in range(1, 4))
    offset = col - 40 * group
    diff = row - offset + 2 * HW
    source = base - 2 * HW + offset
    total = jnp.zeros((8, 160), F32)
    for t in range(TAPS):
        middle = base + row + t - HW
        valid = jnp.logical_and(middle >= 0, middle < NLAT)
        total = total + jnp.where(valid, lat_ref[t] * pick(diff + t, lat_ref), 0.0)
    total = jnp.where(jnp.logical_and(source >= 0, source < NLAT), total, 0.0)
    high, low = split(total)
    blocks = []
    for s in range(2):
        blocks.append(jnp.where((group & 1) == s, high, 0.0))
        blocks.append(jnp.where(group == s, low, 0.0))
    lat_mid[...] = jnp.concatenate(blocks, axis=0).astype(BF16)

    row = iota((8, 192), 0)
    col = iota((8, 192), 1)
    group = sum((col >= 24 * n).astype(I32) for n in range(1, 8))
    offset = col - 24 * group
    source = base - HW + offset
    total = pick(row - offset + 2 * HW, lat_ref)
    total = jnp.where(jnp.logical_and(source >= 0, source < NLAT), total, 0.0)
    high, low = split(total)
    blocks = []
    for s in range(4):
        blocks.append(jnp.where((group & 3) == s, high, 0.0))
        blocks.append(jnp.where(group == s, low, 0.0))
    lat_fin[...] = jnp.concatenate(blocks, axis=0).astype(BF16)

    lag = iota((8, LANES), 1) - 2 * HW
    auto = jnp.zeros((8, LANES), F32)
    for t in range(TAPS):
        auto = auto + lon_ref[t] * pick(lag + t, lon_ref)

    def auto_at(n):
        return jnp.sum(jnp.where(lag[:1] == n, auto[:1], 0.0), axis=1, keepdims=True)

    coefficients = [auto_at(n) for n in range(2 * HW + 1)]
    main = iota((LANES, LANES), 0) - iota((LANES, LANES), 1)
    edge = iota((32, LANES), 0)
    edge = jnp.where(edge < EDGE, edge - EDGE, edge + LANES - EDGE) - iota((32, LANES), 1)

    def smooth_twice(distance):
        distance = jnp.abs(distance)
        out = jnp.zeros(distance.shape, F32)
        for n in range(2 * HW + 1):
            out = jnp.where(distance == n, coefficients[n], out)
        return out

    def place(out_ref, main_value, edge_value):
        main_high, main_low = split(main_value)
        edge_high, edge_low = split(edge_value)
        for v in range(4):
            out_ref[v, :LANES, :LANES] = main_high.astype(BF16)
            out_ref[v, :LANES, LANES:] = main_low.astype(BF16)
            out_ref[v, LANES:, :] = jnp.zeros((LANES, 2 * LANES), BF16)
            out_ref[v, LANES + 32 * v : LANES + 32 * (v + 1), :LANES] = edge_high.astype(BF16)
            out_ref[v, LANES + 32 * v : LANES + 32 * (v + 1), LANES:] = edge_low.astype(BF16)

    place(lon_mid, smooth_twice(main), smooth_twice(edge))
    place(lon_fin, pick(HW - main, lon_ref), pick(HW - edge, lon_ref))


def matrices(band, lat_taps, lon_taps):
    smem = whole(pltpu.SMEM)
    return pl.pallas_call(
        matrices_kernel,
        out_shape=(
            jax.ShapeDtypeStruct((32, 160), BF16),
            jax.ShapeDtypeStruct((4, 256, 256), BF16),
            jax.ShapeDtypeStruct((64, 192), BF16),
            jax.ShapeDtypeStruct((4, 256, 256), BF16),
        ),
        in_specs=[smem] * 3,
        out_specs=(whole(),) * 4,
        cost_estimate=pl.CostEstimate(flops=4000000, bytes_accessed=1100000, transcendentals=0),
        name="matrices",
    )(band, lat_taps, lon_taps)


def pack_kernel(e_ref, out_ref):
    row = iota((LANES, LANES), 0)
    col = iota((LANES, LANES), 1)
    inner = col & 31
    source = jnp.where(inner < EDGE, inner + LANES - EDGE, inner - EDGE)
    count = e_ref.shape[0]
    for g in range(2):
        total = None
        for v in range(4):
            choose = jnp.logical_and(row == source, (col >> 5) == v)
            choose = jnp.where(choose, 1.0, 0.0).astype(BF16)
            tile = e_ref[:, 4 * g + v].astype(F32).reshape(count * ROWS, LANES).astype(BF16)
            part = nn(tile, choose)
            total = part if total is None else total + part
        out_ref[:, g] = total.reshape(count, ROWS, LANES).astype(BF16)


def pack(ensemble):
    step = 16
    return pl.pallas_call(
        pack_kernel,
        grid=(MEM // step,),
        out_shape=jax.ShapeDtypeStruct((MEM, 2, ROWS, LANES), BF16),
        in_specs=[pl.BlockSpec((step, LEV, ROWS, LANES), lambda i: (i, 0, 0, 0))],
        out_specs=pl.BlockSpec((step, 2, ROWS, LANES), lambda i: (i, 0, 0, 0)),
        compiler_params=pltpu.CompilerParams(dimension_semantics=ARB),
        cost_estimate=pl.CostEstimate(flops=4000000, bytes_accessed=1600000, transcendentals=0),
        name="pack",
    )(ensemble)


CHUNK = 256
UNROLL = 2


def place_values(acc_ref, row_hot, lane_of, value_of, lane_iota):
    parts_high, parts_low = [], []
    for q in range(4):
        hit = lane_iota == lane_of[q]
        high, low = split(value_of[q])
        parts_high.append(jnp.where(hit, high, 0.0).astype(BF16))
        parts_low.append(jnp.where(hit, low, 0.0).astype(BF16))
    values = jnp.concatenate(
        [jnp.concatenate(parts_high, axis=1), jnp.concatenate(parts_low, axis=1)], axis=0
    )
    acc_ref[...] += nt(row_hot, values)


def hot_rows(row_of, row_iota):
    parts = [jnp.where(row_iota == row_of[q], 1.0, 0.0).astype(BF16) for q in range(4)]
    return jnp.concatenate(parts, axis=1)


def first_kernel(
    count_ref, ref_ref, level_ref, weight_ref, precision_ref, innovation_ref,
    buffer_ref, row_ref, lane_ref, acc_ref,
):
    counts = count_ref[...].astype(F32)
    below = iota((DEV, DEV), 1) <= iota((DEV, DEV), 0)
    ends = nn(jnp.where(below, 1.0, 0.0).astype(BF16), counts.astype(BF16))
    counts = jnp.concatenate([counts] * (CHUNK // LANES), axis=1)
    ends = jnp.concatenate([ends] * (CHUNK // LANES), axis=1)
    acc_ref[...] = jnp.zeros_like(acc_ref)
    row_iota = iota((BUF, CHUNK), 0).astype(F32)
    lane_iota = iota((LANES, CHUNK), 0).astype(F32)

    @pl.loop(0, NOBS // CHUNK, unroll=UNROLL)
    def _(c):
        part = pl.ds(pl.multiple_of(c * CHUNK, CHUNK), CHUNK)
        level = level_ref[:, part]
        low_level = (level & 3).astype(F32)
        high_level = ((level >> 2) * SLOT).astype(F32)
        forced = -(precision_ref[:, part] * innovation_ref[:, part])
        rows, lanes, values = [], [], []
        for q in range(4):
            position = ref_ref[q : q + 1, part].astype(F32)
            passed = position >= ends
            source = jnp.sum(jnp.where(passed, 1.0, 0.0), axis=0, keepdims=True)
            start = jnp.sum(jnp.where(passed, counts, 0.0), axis=0, keepdims=True)
            rows.append(source * 4.0 + low_level)
            lanes.append(high_level + position - start)
            row_ref[q : q + 1, part] = rows[q]
            lane_ref[q : q + 1, part] = lanes[q]
            values.append(weight_ref[q : q + 1, part] * forced)
        place_values(acc_ref, hot_rows(rows, row_iota), lanes, values, lane_iota)

    buffer_ref[...] = acc_ref[:, :LANES] + acc_ref[:, LANES:]


def first(count, ref, level, weight, precision, innovation):
    return pl.pallas_call(
        first_kernel,
        out_shape=(
            jax.ShapeDtypeStruct((BUF, LANES), F32),
            jax.ShapeDtypeStruct((4, NOBS), F32),
            jax.ShapeDtypeStruct((4, NOBS), F32),
        ),
        in_specs=[whole()] * 6,
        out_specs=(whole(),) * 3,
        scratch_shapes=[VMEM((BUF, 2 * LANES), F32)],
        cost_estimate=pl.CostEstimate(flops=40000000, bytes_accessed=600000, transcendentals=0),
        name="first",
    )(count, ref, level, weight, precision, innovation)


def second_kernel(
    incoming_ref, row_ref, lane_ref, weight_ref, precision_ref, innovation_ref, coef_ref,
    buffer_ref, departure_ref, acc_ref,
):
    flipped = incoming_ref[...].T
    high, low = split(flipped)
    table = jnp.concatenate([high, low], axis=0).astype(BF16)
    acc_ref[...] = jnp.zeros_like(acc_ref)
    row_iota = iota((BUF, CHUNK), 0).astype(F32)
    lane_iota = iota((LANES, CHUNK), 0).astype(F32)
    earlier = coef_ref[3, :1, :1]
    later = coef_ref[4, :1, :1]

    @pl.loop(0, NOBS // CHUNK, unroll=UNROLL)
    def _(c):
        part = pl.ds(pl.multiple_of(c * CHUNK, CHUNK), CHUNK)
        rows = [row_ref[q : q + 1, part] for q in range(4)]
        lanes = [lane_ref[q : q + 1, part] for q in range(4)]
        weights = [weight_ref[q : q + 1, part] for q in range(4)]
        innovation = innovation_ref[:, part]
        row_hot = hot_rows(rows, row_iota)
        found = nn(table, row_hot)
        found = found[:LANES] + found[LANES:]
        departure = -innovation
        for q in range(4):
            column = found[:, q * CHUNK : (q + 1) * CHUNK]
            picked = jnp.sum(jnp.where(lane_iota == lanes[q], column, 0.0), axis=0, keepdims=True)
            departure = departure + weights[q] * picked
        departure_ref[:, part] = departure
        forced = precision_ref[:, part] * (later * departure - earlier * innovation)
        values = [weights[q] * forced for q in range(4)]
        place_values(acc_ref, row_hot, lanes, values, lane_iota)

    buffer_ref[...] = acc_ref[:, :LANES] + acc_ref[:, LANES:]


def second(incoming, rows, lanes, weight, precision, innovation, coefs):
    return pl.pallas_call(
        second_kernel,
        out_shape=(
            jax.ShapeDtypeStruct((BUF, LANES), F32),
            jax.ShapeDtypeStruct((1, NOBS), F32),
        ),
        in_specs=[whole()] * 7,
        out_specs=(whole(),) * 2,
        scratch_shapes=[VMEM((BUF, 2 * LANES), F32)],
        cost_estimate=pl.CostEstimate(flops=60000000, bytes_accessed=800000, transcendentals=0),
        name="second",
    )(incoming, rows, lanes, weight, precision, innovation, coefs)


def swap_quadrants(tile):
    sub = iota((8, LANES), 0) < 4
    lane = iota((8, LANES), 1) < SLOT
    moved = pltpu.roll(pltpu.roll(tile, 4, 0), SLOT, 1)
    return jnp.where(sub == lane, tile, moved)


PAIRS = DEV // 2
GROUP = 4


def columns_kernel(buffer_ref, cell_ref, out_ref, grid_ref):
    lane_iota = iota((LANES, LANES), 0)
    total = jnp.zeros((LANES, LANES), F32)
    for n in range(0, PAIRS, GROUP):
        values, hots = [], []
        for m in range(n, n + GROUP):
            tile = swap_quadrants(buffer_ref[8 * m : 8 * m + 8, :])
            cell = cell_ref[m : m + 1, :]
            row = cell >> 7
            high, low = split(tile)
            masks = [row == r for r in range(ROWS)]
            values.append(
                jnp.concatenate(
                    [jnp.where(k, high, 0.0) for k in masks] + [jnp.where(k, low, 0.0) for k in masks],
                    axis=0,
                ).astype(BF16)
            )
            hots.append(jnp.where(lane_iota == (cell & 127), 1.0, 0.0).astype(BF16))
        total = total + nt(jnp.concatenate(values, axis=1), jnp.concatenate(hots, axis=1))

    grid_ref[...] = total[:64] + total[64:]
    lane = iota((ROWS, LANES), 1)
    inner = lane & 31
    edges = [jnp.zeros((ROWS, LANES), F32)] * 2
    for l in range(LEV):
        tile = grid_ref[pl.ds(l, ROWS, stride=LEV), :]
        out_ref[l] = tile
        v = l % 4
        right = pltpu.roll(tile, (32 * v + EDGE) % LANES, 1)
        left = pltpu.roll(tile, (32 * v + EDGE) % LANES, 1)
        moved = jnp.where(inner < EDGE, right, left)
        edges[l // 4] = jnp.where((lane >> 5) == v, moved, edges[l // 4])
    out_ref[LEV] = edges[0]
    out_ref[LEV + 1] = edges[1]


def columns(buffer, cells):
    return pl.pallas_call(
        columns_kernel,
        out_shape=jax.ShapeDtypeStruct((LEV + 2, ROWS, LANES), F32),
        in_specs=[whole()] * 2,
        out_specs=whole(),
        scratch_shapes=[VMEM((64, LANES), F32)],
        cost_estimate=pl.CostEstimate(flops=20000000, bytes_accessed=400000, transcendentals=0),
        name="columns",
    )(buffer, cells)


def slots_kernel(increment_ref, cell_ref, out_ref):
    rows = [increment_ref[pl.ds(r, LEV, stride=ROWS), :] for r in range(ROWS)]
    pairs = [split(value) for value in rows]
    table = jnp.concatenate([p[0] for p in pairs] + [p[1] for p in pairs], axis=0).astype(BF16)
    lane_iota = iota((LANES, LANES), 0)

    for n in range(0, PAIRS, GROUP):
        hots, cells = [], []
        for m in range(n, n + GROUP):
            cell = cell_ref[m : m + 1, :]
            cells.append(cell >> 7)
            hots.append(jnp.where(lane_iota == (cell & 127), 1.0, 0.0).astype(BF16))
        found = nn(table, jnp.concatenate(hots, axis=1))
        found = found[:64] + found[64:]
        for g in range(GROUP):
            tile = jnp.zeros((LEV, LANES), F32)
            for r in range(ROWS):
                part = found[8 * r : 8 * r + 8, g * LANES : (g + 1) * LANES]
                tile = jnp.where(cells[g] == r, part, tile)
            out_ref[8 * (n + g) : 8 * (n + g) + 8, :] = swap_quadrants(tile)


def slots(increment, cells):
    return pl.pallas_call(
        slots_kernel,
        out_shape=jax.ShapeDtypeStruct((BUF, LANES), F32),
        in_specs=[whole()] * 2,
        out_specs=whole(),
        cost_estimate=pl.CostEstimate(flops=20000000, bytes_accessed=400000, transcendentals=0),
        name="slots",
    )(increment, cells)


def row_pass(e_refs, fields, lat_ref, stack, out_ref, lane0):
    per = MEM // stack
    wide = 2
    lat = lat_ref[...]

    def column_of(tiles):
        value = jnp.concatenate(tiles, axis=0)
        high = value.astype(BF16)
        low = (value - high.astype(F32)).astype(BF16)
        return jnp.concatenate([high, low], axis=0)

    def store(row, value):
        high = value.astype(BF16)
        out_ref[0, row : row + 16, lane0 : lane0 + LANES] = high
        low = (value - high.astype(F32)).astype(BF16)
        out_ref[1, row : row + 16, lane0 : lane0 + LANES] = low

    def block(value, s, n):
        tile = value[16 * s : 16 * s + 16, n * LANES : (n + 1) * LANES]
        return tile[:8] + tile[8:]

    for c in range(0, per, wide):
        parts = []
        for n in range(c, c + wide):
            tiles = []
            for s in range(stack):
                tiles += [e[s * per + n, 0].astype(F32) * f for e, f in zip(e_refs, fields)]
            parts.append(column_of(tiles))
        value = nn(lat, jnp.concatenate(parts, axis=1))
        for s in range(stack):
            for n in range(0, wide, 2):
                pair = jnp.concatenate([block(value, s, n), block(value, s, n + 1)], axis=0)
                store((s * per + c + n) * 8, pair)

    blank = [jnp.zeros((ROWS, LANES), F32)] * (len(fields) * (stack - 1))
    one = block(nn(lat, column_of(list(fields) + blank)), 0, 0)
    store(MEM * 8, jnp.concatenate([one, jnp.zeros_like(one)], axis=0))


def column_pass(in_ref, weights, start, size):
    value = nn(in_ref[0, start : start + size, :], weights)
    value = value + nn(in_ref[1, start : start + size, :], weights)
    return value[:, :LANES] + value[:, LANES:]


def merge_edges(left, right):
    inner = iota((ROWS, LANES), 1) & 31
    return jnp.where(inner < EDGE, left, right)


def middle_kernel(*refs):
    e_refs = refs[:5]
    h_refs = refs[5:10]
    f_refs = refs[10:15]
    left_ref, right_ref, lat_ref, lon_ref, coef_ref, out_ref, pass_ref = refs[15:]
    l = pl.program_id(0)

    @pl.when((l & 3) == 0)
    def _():
        g = l >> 2
        fields = [merge_edges(left_ref[x, g], right_ref[x, g]) for x in range(5)]
        row_pass(h_refs, fields, lat_ref, 2, pass_ref, LANES)

    fields = [f_refs[x][l] for x in range(5)]
    row_pass(e_refs, fields, lat_ref, 2, pass_ref, 0)
    weights = lon_ref[0]
    step = 16

    total = jnp.zeros((ROWS, LANES), F32)
    for c in range(MEM // step):
        value = column_pass(pass_ref, weights, c * 8 * step, 8 * step)
        for k in range(step):
            own = e_refs[2][c * step + k, 0].astype(F32)
            total = total + value[8 * k : 8 * k + 8] * own
    single = column_pass(pass_ref, weights, MEM * 8, 16)[:8]
    out_ref[0] = coef_ref[0] * total + coef_ref[1, pl.ds(l, 1), :] * single


def level_block(count):
    return pl.BlockSpec((count, 1, ROWS, LANES), lambda l: (0, l, 0, 0))


def edge_block(count):
    return pl.BlockSpec((count, 1, ROWS, LANES), lambda l: (0, l // 4, 0, 0))


def middle(members, halos, fields, left, right, lat_mid, lon_mid, coefs):
    return pl.pallas_call(
        middle_kernel,
        grid=(LEV,),
        out_shape=jax.ShapeDtypeStruct((LEV, ROWS, LANES), F32),
        in_specs=[level_block(MEM)] * 5
        + [edge_block(MEM)] * 5
        + [whole()] * 8
        + [pl.BlockSpec((1, 256, 256), lambda l: (l % 4, 0, 0)), whole()],
        out_specs=pl.BlockSpec((1, ROWS, LANES), lambda l: (l, 0, 0)),
        scratch_shapes=[VMEM((2, MEM * 8 + 16, 256), BF16)],
        compiler_params=pltpu.CompilerParams(dimension_semantics=ARB),
        cost_estimate=pl.CostEstimate(flops=100000000, bytes_accessed=9000000, transcendentals=0),
        name="middle",
    )(*members, *halos, *fields, left, right, lat_mid, lon_mid, coefs)


def final_kernel(*refs):
    e_refs = refs[:3]
    h_refs = refs[3:6]
    f_refs = refs[6:9]
    left_ref, right_ref, lat_ref, lon_ref, coef_ref, out_ref, static_ref, pass_ref = refs[9:]
    l = pl.program_id(0)

    @pl.when((l & 3) == 0)
    def _():
        g = l >> 2
        fields = [merge_edges(left_ref[x, g], right_ref[x, g]) for x in range(3)]
        row_pass(h_refs, fields, lat_ref, 4, pass_ref, LANES)

    fields = [f_refs[x][l] for x in range(3)]
    row_pass(e_refs, fields, lat_ref, 4, pass_ref, 0)
    weights = lon_ref[0]
    step = 16
    scale = -HYBRID_ENSEMBLE / math.sqrt(MEM - 1)

    for c in range(MEM // step):
        value = column_pass(pass_ref, weights, c * 8 * step, 8 * step)
        out_ref[c * step : (c + 1) * step, 0] = (scale * value).reshape(step, ROWS, LANES)

    single = column_pass(pass_ref, weights, MEM * 8, 16)[:8]
    static_ref[0] = coef_ref[2, pl.ds(l, 1), :] * single


def final(members, halos, fields, left, right, lat_fin, lon_fin, coefs):
    return pl.pallas_call(
        final_kernel,
        grid=(LEV,),
        out_shape=(
            jax.ShapeDtypeStruct((MEM, LEV, ROWS, LANES), F32),
            jax.ShapeDtypeStruct((LEV, ROWS, LANES), F32),
        ),
        in_specs=[level_block(MEM)] * 3
        + [edge_block(MEM)] * 3
        + [whole()] * 6
        + [pl.BlockSpec((1, 256, 256), lambda l: (l % 4, 0, 0)), whole()],
        out_specs=(level_block(MEM), pl.BlockSpec((1, ROWS, LANES), lambda l: (l, 0, 0))),
        scratch_shapes=[VMEM((2, MEM * 8 + 16, 256), BF16)],
        compiler_params=pltpu.CompilerParams(dimension_semantics=ARB),
        cost_estimate=pl.CostEstimate(flops=100000000, bytes_accessed=9000000, transcendentals=0),
        name="final",
    )(*members, *halos, *fields, left, right, lat_fin, lon_fin, coefs)


def shift(value, axis, step):
    count = lax.axis_size(axis)
    return lax.ppermute(value, axis, [(i, (i + step) % count) for i in range(count)])


def edges_kernel(*refs):
    for x, ref in enumerate(refs[:-1]):
        refs[-1][x] = ref[LEV:]


def surround(forcing, reach):
    bands = range(reach, -reach - 1, -1)
    fields = [shift(forcing, "lat", d) if d else forcing for d in bands]
    edges = pl.pallas_call(
        edges_kernel,
        out_shape=jax.ShapeDtypeStruct((len(fields), 2, ROWS, LANES), F32),
        in_specs=[whole()] * len(fields),
        out_specs=whole(),
        cost_estimate=pl.CostEstimate(flops=100000, bytes_accessed=100000, transcendentals=0),
        name="edges",
    )(*fields)
    return fields, shift(edges, "lon", 1), shift(edges, "lon", -1)


def route(buffer):
    buffer = buffer.reshape(DEV, 4, LANES)
    out = lax.all_to_all(buffer, ("lat", "lon"), split_axis=0, concat_axis=0, tiled=True)
    return out.reshape(BUF, LANES)


def per_device(
    ensemble,
    static_sigma,
    lat_taps,
    lon_taps,
    step_len,
    send_cols,
    send_count,
    obs_ref,
    obs_level,
    obs_weight,
    innovation,
    obs_precision,
):
    ens_scale = HYBRID_ENSEMBLE / math.sqrt(MEM - 1)
    counts = jnp.broadcast_to(send_count.reshape(DEV, 1, 1), (DEV, 1, LANES))
    received = lax.all_to_all(counts, ("lat", "lon"), split_axis=0, concat_axis=0, tiled=True)
    received = received.reshape(DEV, LANES)
    cells = send_cols.reshape(PAIRS, LANES)
    level = obs_level.reshape(1, NOBS)
    ref = obs_ref.reshape(4, NOBS)
    weight = obs_weight.reshape(4, NOBS)
    innov = innovation.reshape(1, NOBS)
    precision = obs_precision.reshape(1, NOBS)

    ones = jnp.ones((LEV, LANES), F32)
    sigma = static_sigma[:, None] * ones
    coefs = jnp.stack(
        [
            (-step_len[0] * ens_scale * ens_scale) * ones,
            (-step_len[0] * HYBRID_STATIC * HYBRID_STATIC) * sigma * sigma,
            -HYBRID_STATIC * sigma,
            ((1.0 - step_len[1]) * step_len[0]) * ones,
            step_len[1] * ones,
        ]
    )
    band = lax.axis_index("lat").astype(I32).reshape(1)
    lat_mid, lon_mid, lat_fin, lon_fin = matrices(band, lat_taps, lon_taps)

    north = shift(ensemble, "lat", 1)
    south = shift(ensemble, "lat", -1)
    packed = pack(ensemble)
    from_left = shift(packed, "lon", 1)
    from_right = shift(packed, "lon", -1)
    inner = lax.broadcasted_iota(I32, packed.shape, 3) & 31
    halo = jnp.where(inner < EDGE, from_left, from_right)
    north2 = shift(north, "lat", 1)
    south2 = shift(south, "lat", -1)
    halo_n = shift(halo, "lat", 1)
    halo_s = shift(halo, "lat", -1)
    halo_n2 = shift(halo_n, "lat", 1)
    halo_s2 = shift(halo_s, "lat", -1)
    members = [north2, north, ensemble, south, south2]
    halos = [halo_n2, halo_n, halo, halo_s, halo_s2]

    outgoing, rows, lanes = first(received, ref, level, weight, precision, innov)
    arrived = route(outgoing)
    forcing = columns(arrived, cells)
    around = surround(forcing, 2)
    increment = middle(members, halos, *around, lat_mid, lon_mid, coefs)
    incoming = route(slots(increment.reshape(LEV * ROWS, LANES), cells))
    outgoing, departure = second(incoming, rows, lanes, weight, precision, innov, coefs)
    around = surround(columns(route(outgoing), cells), 1)
    control, static = final(members[1:4], halos[1:4], *around, lat_fin, lon_fin, coefs)
    return (control, static, departure.reshape(1, 1, -1))


def solution(mesh):
    return jax.shard_map(
        per_device,
        mesh=mesh,
        in_specs=(
            P(None, None, "lat", "lon"),
            P(),
            P(),
            P(),
            P(),
            P("lat", "lon", None, None),
            P("lat", "lon", None),
            P("lat", "lon", None, None),
            P("lat", "lon", None),
            P("lat", "lon", None, None),
            P("lat", "lon", None),
            P("lat", "lon", None),
        ),
        out_specs=(P(None, None, "lat", "lon"), P(None, "lat", "lon"), P("lat", "lon", None)),
        check_vma=False,
    )
```

```python
import functools
import math

import jax
import jax.numpy as jnp
from jax import lax
from jax.experimental import pallas as pl
from jax.experimental.pallas import tpu as pltpu
from jax.sharding import PartitionSpec as P


HYBRID_STATIC = 0.5
HYBRID_ENSEMBLE = 0.8660254037844386
F32 = jnp.float32
BF16 = jnp.bfloat16
I32 = jnp.int32

MEM = 80
LEV = 8
ROWS = 8
LANES = 128
NOBS = 2048
SLOT = 64
DEV = 128
NLAT = 64
HW = 8
TAPS = 17
EDGE = 16
BUF = DEV * 4
PAIRS = DEV // 2

VMEM = pltpu.VMEM
ARB = ("arbitrary",)


def whole(memory_space=VMEM):
    return pl.BlockSpec(memory_space=memory_space)


def near(*arrays):
    return [pltpu.with_memory_space_constraint(a, VMEM) for a in arrays]


def split(value):
    high = value.astype(BF16).astype(F32)
    return high, value - high


def iota(shape, dim):
    return lax.broadcasted_iota(I32, shape, dim)


def nn(a, b):
    return lax.dot_general(a, b, (((1,), (0,)), ((), ())), preferred_element_type=F32)


def nt(a, b):
    return lax.dot_general(a, b, (((1,), (1,)), ((), ())), preferred_element_type=F32)


def matrices_kernel(
    band_ref, lat_ref, lon_ref, sigma_ref, step_ref, cols_ref,
    lat_mid, lon_mid, lat_fin, lon_fin, coef_ref, cell_ref,
):
    base = band_ref[0] * ROWS
    cell_ref[...] = jnp.concatenate(
        [cols_ref[pl.ds(h, PAIRS, stride=2), :] for h in range(2)], axis=1
    )
    ens_scale = HYBRID_ENSEMBLE / math.sqrt(MEM - 1)
    level = iota((LEV, LANES), 0)
    sigma = jnp.zeros((LEV, LANES), F32)
    for l in range(LEV):
        sigma = jnp.where(level == l, sigma_ref[l], sigma)
    once = jnp.ones((LEV, LANES), F32)
    step0 = once * step_ref[0]
    step1 = once * step_ref[1]
    coef_ref[0] = step0 * (-ens_scale * ens_scale)
    coef_ref[1] = step0 * sigma * sigma * (-HYBRID_STATIC * HYBRID_STATIC)
    coef_ref[2] = sigma * -HYBRID_STATIC
    coef_ref[3] = (1.0 - step1) * step0
    coef_ref[4] = step1

    def pick(index, taps):
        out = jnp.zeros(index.shape, F32)
        for t in range(TAPS):
            out = jnp.where(index == t, taps[t], out)
        return out

    row = iota((8, 160), 0)
    col = iota((8, 160), 1)
    group = sum((col >= 40 * n).astype(I32) for n in range(1, 4))
    offset = col - 40 * group
    diff = row - offset + 2 * HW
    source = base - 2 * HW + offset
    total = jnp.zeros((8, 160), F32)
    for t in range(TAPS):
        middle = base + row + t - HW
        valid = jnp.logical_and(middle >= 0, middle < NLAT)
        total = total + jnp.where(valid, lat_ref[t] * pick(diff + t, lat_ref), 0.0)
    total = jnp.where(jnp.logical_and(source >= 0, source < NLAT), total, 0.0)
    high, low = split(total)
    blocks = []
    for s in range(2):
        blocks.append(jnp.where((group & 1) == s, high, 0.0))
        blocks.append(jnp.where(group == s, low, 0.0))
    lat_mid[...] = jnp.concatenate(blocks, axis=0).astype(BF16)

    row = iota((8, 192), 0)
    col = iota((8, 192), 1)
    group = sum((col >= 24 * n).astype(I32) for n in range(1, 8))
    offset = col - 24 * group
    source = base - HW + offset
    total = pick(row - offset + 2 * HW, lat_ref)
    total = jnp.where(jnp.logical_and(source >= 0, source < NLAT), total, 0.0)
    high, low = split(total)
    blocks = []
    for s in range(4):
        blocks.append(jnp.where((group & 3) == s, high, 0.0))
        blocks.append(jnp.where(group == s, low, 0.0))
    lat_fin[...] = jnp.concatenate(blocks, axis=0).astype(BF16)

    lag = iota((8, LANES), 1) - 2 * HW
    auto = jnp.zeros((8, LANES), F32)
    for t in range(TAPS):
        auto = auto + lon_ref[t] * pick(lag + t, lon_ref)

    def auto_at(n):
        return jnp.sum(jnp.where(lag[:1] == n, auto[:1], 0.0), axis=1, keepdims=True)

    coefficients = [auto_at(n) for n in range(2 * HW + 1)]
    main = iota((LANES, LANES), 0) - iota((LANES, LANES), 1)
    edge = iota((32, LANES), 0)
    edge = jnp.where(edge < EDGE, edge - EDGE, edge + LANES - EDGE) - iota((32, LANES), 1)

    def smooth_twice(distance):
        distance = jnp.abs(distance)
        out = jnp.zeros(distance.shape, F32)
        for n in range(2 * HW + 1):
            out = jnp.where(distance == n, coefficients[n], out)
        return out

    def place(out_ref, main_value, edge_value):
        main_high, main_low = split(main_value)
        edge_high, edge_low = split(edge_value)
        for v in range(4):
            out_ref[v, :LANES, :LANES] = main_high.astype(BF16)
            out_ref[v, :LANES, LANES:] = main_low.astype(BF16)
            out_ref[v, LANES:, :] = jnp.zeros((LANES, 2 * LANES), BF16)
            out_ref[v, LANES + 32 * v : LANES + 32 * (v + 1), :LANES] = edge_high.astype(BF16)
            out_ref[v, LANES + 32 * v : LANES + 32 * (v + 1), LANES:] = edge_low.astype(BF16)

    place(lon_mid, smooth_twice(main), smooth_twice(edge))
    place(lon_fin, pick(HW - main, lon_ref), pick(HW - edge, lon_ref))


def matrices(band, lat_taps, lon_taps, static_sigma, step_len, cols):
    smem = whole(pltpu.SMEM)
    return pl.pallas_call(
        matrices_kernel,
        out_shape=(
            jax.ShapeDtypeStruct((32, 160), BF16),
            jax.ShapeDtypeStruct((4, 256, 256), BF16),
            jax.ShapeDtypeStruct((64, 192), BF16),
            jax.ShapeDtypeStruct((4, 256, 256), BF16),
            jax.ShapeDtypeStruct((5, LEV, LANES), F32),
            jax.ShapeDtypeStruct((PAIRS, LANES), I32),
        ),
        in_specs=[smem] * 5 + [whole()],
        out_specs=(whole(),) * 6,
        cost_estimate=pl.CostEstimate(flops=4000000, bytes_accessed=1100000, transcendentals=0),
        name="matrices",
    )(band, lat_taps, lon_taps, static_sigma, step_len, cols)


def pack_kernel(e_ref, out_ref):
    row = iota((LANES, LANES), 0)
    col = iota((LANES, LANES), 1)
    inner = col & 31
    source = jnp.where(inner < EDGE, inner + LANES - EDGE, inner - EDGE)
    count = e_ref.shape[0]
    for g in range(2):
        total = None
        for v in range(4):
            choose = jnp.logical_and(row == source, (col >> 5) == v)
            choose = jnp.where(choose, 1.0, 0.0).astype(BF16)
            tile = e_ref[:, 4 * g + v].astype(F32).reshape(count * ROWS, LANES).astype(BF16)
            part = nn(tile, choose)
            total = part if total is None else total + part
        out_ref[:, g] = total.reshape(count, ROWS, LANES).astype(BF16)


def pack(ensemble):
    step = 16
    return pl.pallas_call(
        pack_kernel,
        grid=(MEM // step,),
        out_shape=jax.ShapeDtypeStruct((MEM, 2, ROWS, LANES), BF16),
        in_specs=[pl.BlockSpec((step, LEV, ROWS, LANES), lambda i: (i, 0, 0, 0))],
        out_specs=pl.BlockSpec((step, 2, ROWS, LANES), lambda i: (i, 0, 0, 0)),
        compiler_params=pltpu.CompilerParams(dimension_semantics=ARB),
        cost_estimate=pl.CostEstimate(flops=4000000, bytes_accessed=1600000, transcendentals=0),
        name="pack",
    )(ensemble)


CHUNK = 256
UNROLL = 2


def place_values(acc_ref, row_hot, lane_of, value_of, lane_iota):
    parts_high, parts_low = [], []
    for q in range(4):
        hit = lane_iota == lane_of[q]
        high, low = split(value_of[q])
        parts_high.append(jnp.where(hit, high, 0.0).astype(BF16))
        parts_low.append(jnp.where(hit, low, 0.0).astype(BF16))
    values = jnp.concatenate(
        [jnp.concatenate(parts_high, axis=1), jnp.concatenate(parts_low, axis=1)], axis=0
    )
    acc_ref[...] += nt(row_hot, values)


def hot_rows(row_of, row_iota):
    parts = [jnp.where(row_iota == row_of[q], 1.0, 0.0).astype(BF16) for q in range(4)]
    return jnp.concatenate(parts, axis=1)


def first_kernel(
    count_ref, ref_ref, level_ref, weight_ref, precision_ref, innovation_ref,
    buffer_ref, row_ref, lane_ref, acc_ref,
):
    counts = count_ref[...].astype(F32)
    below = iota((DEV, DEV), 1) <= iota((DEV, DEV), 0)
    ends = nn(jnp.where(below, 1.0, 0.0).astype(BF16), counts.astype(BF16))
    counts = jnp.concatenate([counts] * (CHUNK // LANES), axis=1)
    ends = jnp.concatenate([ends] * (CHUNK // LANES), axis=1)
    acc_ref[...] = jnp.zeros_like(acc_ref)
    row_iota = iota((BUF, CHUNK), 0).astype(F32)
    lane_iota = iota((LANES, CHUNK), 0).astype(F32)

    @pl.loop(0, NOBS // CHUNK, unroll=UNROLL)
    def _(c):
        part = pl.ds(pl.multiple_of(c * CHUNK, CHUNK), CHUNK)
        level = level_ref[:, part]
        low_level = (level & 3).astype(F32)
        high_level = ((level >> 2) * SLOT).astype(F32)
        forced = -(precision_ref[:, part] * innovation_ref[:, part])
        rows, lanes, values = [], [], []
        for q in range(4):
            position = ref_ref[q : q + 1, part].astype(F32)
            passed = position >= ends
            source = jnp.sum(jnp.where(passed, 1.0, 0.0), axis=0, keepdims=True)
            start = jnp.sum(jnp.where(passed, counts, 0.0), axis=0, keepdims=True)
            rows.append(source * 4.0 + low_level)
            lanes.append(high_level + position - start)
            row_ref[q : q + 1, part] = rows[q]
            lane_ref[q : q + 1, part] = lanes[q]
            values.append(weight_ref[q : q + 1, part] * forced)
        place_values(acc_ref, hot_rows(rows, row_iota), lanes, values, lane_iota)

    buffer_ref[...] = acc_ref[:, :LANES] + acc_ref[:, LANES:]


def first(count, ref, level, weight, precision, innovation):
    return pl.pallas_call(
        first_kernel,
        out_shape=(
            jax.ShapeDtypeStruct((BUF, LANES), F32),
            jax.ShapeDtypeStruct((4, NOBS), F32),
            jax.ShapeDtypeStruct((4, NOBS), F32),
        ),
        in_specs=[whole()] * 6,
        out_specs=(whole(),) * 3,
        scratch_shapes=[VMEM((BUF, 2 * LANES), F32)],
        cost_estimate=pl.CostEstimate(flops=40000000, bytes_accessed=600000, transcendentals=0),
        name="first",
    )(*near(count), ref, level, weight, precision, innovation)


def second_kernel(
    incoming_ref, row_ref, lane_ref, weight_ref, precision_ref, innovation_ref, coef_ref,
    buffer_ref, departure_ref, acc_ref,
):
    flipped = incoming_ref[...].T
    high, low = split(flipped)
    table = jnp.concatenate([high, low], axis=0).astype(BF16)
    acc_ref[...] = jnp.zeros_like(acc_ref)
    row_iota = iota((BUF, CHUNK), 0).astype(F32)
    lane_iota = iota((LANES, CHUNK), 0).astype(F32)
    earlier = coef_ref[3, :1, :1]
    later = coef_ref[4, :1, :1]

    @pl.loop(0, NOBS // CHUNK, unroll=1)
    def _(c):
        part = pl.ds(pl.multiple_of(c * CHUNK, CHUNK), CHUNK)
        rows = [row_ref[q : q + 1, part] for q in range(4)]
        lanes = [lane_ref[q : q + 1, part] for q in range(4)]
        weights = [weight_ref[q : q + 1, part] for q in range(4)]
        innovation = innovation_ref[:, part]
        row_hot = hot_rows(rows, row_iota)
        found = nn(table, row_hot)
        found = found[:LANES] + found[LANES:]
        departure = -innovation
        for q in range(4):
            column = found[:, q * CHUNK : (q + 1) * CHUNK]
            picked = jnp.sum(jnp.where(lane_iota == lanes[q], column, 0.0), axis=0, keepdims=True)
            departure = departure + weights[q] * picked
        departure_ref[:, part] = departure
        forced = precision_ref[:, part] * (later * departure - earlier * innovation)
        values = [weights[q] * forced for q in range(4)]
        place_values(acc_ref, row_hot, lanes, values, lane_iota)

    buffer_ref[...] = acc_ref[:, :LANES] + acc_ref[:, LANES:]


def second(incoming, rows, lanes, weight, precision, innovation, coefs):
    return pl.pallas_call(
        second_kernel,
        out_shape=(
            jax.ShapeDtypeStruct((BUF, LANES), F32),
            jax.ShapeDtypeStruct((1, NOBS), F32),
        ),
        in_specs=[whole()] * 7,
        out_specs=(whole(),) * 2,
        scratch_shapes=[VMEM((BUF, 2 * LANES), F32)],
        cost_estimate=pl.CostEstimate(flops=60000000, bytes_accessed=800000, transcendentals=0),
        name="second",
    )(*near(incoming, rows, lanes), weight, precision, innovation, *near(coefs))


def swap_quadrants(tile):
    sub = iota((8, LANES), 0) < 4
    lane = iota((8, LANES), 1) < SLOT
    moved = pltpu.roll(pltpu.roll(tile, 4, 0), SLOT, 1)
    return jnp.where(sub == lane, tile, moved)


GROUP = 4


def columns_kernel(buffer_ref, cell_ref, out_ref, grid_ref):
    lane_iota = iota((LANES, LANES), 0)
    total = jnp.zeros((LANES, LANES), F32)
    for n in range(0, PAIRS, GROUP):
        values, hots = [], []
        for m in range(n, n + GROUP):
            tile = swap_quadrants(buffer_ref[8 * m : 8 * m + 8, :])
            cell = cell_ref[m : m + 1, :]
            row = cell >> 7
            high, low = split(tile)
            masks = [row == r for r in range(ROWS)]
            values.append(
                jnp.concatenate(
                    [jnp.where(k, high, 0.0) for k in masks] + [jnp.where(k, low, 0.0) for k in masks],
                    axis=0,
                ).astype(BF16)
            )
            hots.append(jnp.where(lane_iota == (cell & 127), 1.0, 0.0).astype(BF16))
        total = total + nt(jnp.concatenate(values, axis=1), jnp.concatenate(hots, axis=1))

    grid_ref[...] = total[:64] + total[64:]
    lane = iota((ROWS, LANES), 1)
    inner = lane & 31
    edges = [jnp.zeros((ROWS, LANES), F32)] * 2
    for l in range(LEV):
        tile = grid_ref[pl.ds(l, ROWS, stride=LEV), :]
        out_ref[l] = tile
        v = l % 4
        right = pltpu.roll(tile, (32 * v + EDGE) % LANES, 1)
        left = pltpu.roll(tile, (32 * v + EDGE) % LANES, 1)
        moved = jnp.where(inner < EDGE, right, left)
        edges[l // 4] = jnp.where((lane >> 5) == v, moved, edges[l // 4])
    out_ref[LEV] = edges[0]
    out_ref[LEV + 1] = edges[1]


def columns(buffer, cells):
    return pl.pallas_call(
        columns_kernel,
        out_shape=jax.ShapeDtypeStruct((LEV + 2, ROWS, LANES), F32),
        in_specs=[whole()] * 2,
        out_specs=whole(),
        scratch_shapes=[VMEM((64, LANES), F32)],
        cost_estimate=pl.CostEstimate(flops=20000000, bytes_accessed=400000, transcendentals=0),
        name="columns",
    )(*near(buffer, cells))


def slots_kernel(increment_ref, cell_ref, out_ref):
    rows = [increment_ref[pl.ds(r, LEV, stride=ROWS), :] for r in range(ROWS)]
    pairs = [split(value) for value in rows]
    table = jnp.concatenate([p[0] for p in pairs] + [p[1] for p in pairs], axis=0).astype(BF16)
    lane_iota = iota((LANES, LANES), 0)

    for n in range(0, PAIRS, GROUP):
        hots, cells = [], []
        for m in range(n, n + GROUP):
            cell = cell_ref[m : m + 1, :]
            cells.append(cell >> 7)
            hots.append(jnp.where(lane_iota == (cell & 127), 1.0, 0.0).astype(BF16))
        found = nn(table, jnp.concatenate(hots, axis=1))
        found = found[:64] + found[64:]
        for g in range(GROUP):
            tile = jnp.zeros((LEV, LANES), F32)
            for r in range(ROWS):
                part = found[8 * r : 8 * r + 8, g * LANES : (g + 1) * LANES]
                tile = jnp.where(cells[g] == r, part, tile)
            out_ref[8 * (n + g) : 8 * (n + g) + 8, :] = swap_quadrants(tile)


def slots(increment, cells):
    return pl.pallas_call(
        slots_kernel,
        out_shape=jax.ShapeDtypeStruct((BUF, LANES), F32),
        in_specs=[whole()] * 2,
        out_specs=whole(),
        cost_estimate=pl.CostEstimate(flops=20000000, bytes_accessed=400000, transcendentals=0),
        name="slots",
    )(*near(increment, cells))


STEP = 16


def column_of(tiles):
    value = jnp.concatenate(tiles, axis=0)
    high = value.astype(BF16)
    low = (value - high.astype(F32)).astype(BF16)
    return jnp.concatenate([high, low], axis=0)


def halves(value):
    high = value.astype(BF16)
    return high, (value - high.astype(F32)).astype(BF16)


def block(value, s, n):
    tile = value[16 * s : 16 * s + 16, n * LANES : (n + 1) * LANES]
    return tile[:8] + tile[8:]


def filter_rows(tiles_of, fields, lat, stack):
    per = STEP // stack
    out = [None] * STEP
    for c in range(0, per, 2):
        parts = []
        for n in range(c, c + 2):
            tiles = []
            for s in range(stack):
                tiles += [t * f for t, f in zip(tiles_of(s * per + n), fields)]
            parts.append(column_of(tiles))
        value = nn(lat, jnp.concatenate(parts, axis=1))
        for s in range(stack):
            for n in range(2):
                out[s * per + c + n] = block(value, s, n)
    return halves(jnp.concatenate(out, axis=0))


def filter_single(fields, lat, stack):
    blank = [jnp.zeros((ROWS, LANES), F32)] * (len(fields) * (stack - 1))
    return block(nn(lat, column_of(list(fields) + blank)), 0, 0)


def filter_columns(high, low, weights):
    value = nn(high, weights) + nn(low, weights)
    return value[:, :LANES] + value[:, LANES:]


def rows_kernel(count, stack, *refs):
    e_refs = refs[:count]
    f_refs = refs[count : 2 * count]
    lat_ref, out_ref, static_ref = refs[2 * count :]
    lat = lat_ref[...]

    @pl.when(pl.program_id(0) == 0)
    def _():
        for l in range(LEV):
            static_ref[l] = filter_single([f[l] for f in f_refs], lat, stack)

    for l in range(LEV):
        high, low = filter_rows(
            lambda k: [e[k, l].astype(F32) for e in e_refs], [f[l] for f in f_refs], lat, stack
        )
        out_ref[0, l, 0] = high
        out_ref[0, l, 1] = low


def member_block(depth):
    return pl.BlockSpec((STEP, depth, ROWS, LANES), lambda i: (i, 0, 0, 0))


def pass_block():
    return pl.BlockSpec((1, LEV, 2, STEP * ROWS, LANES), lambda i: (i, 0, 0, 0, 0))


def filtered(members, fields, lat, stack):
    count = len(members)
    return pl.pallas_call(
        functools.partial(rows_kernel, count, stack),
        grid=(MEM // STEP,),
        out_shape=(
            jax.ShapeDtypeStruct((MEM // STEP, LEV, 2, STEP * ROWS, LANES), BF16),
            jax.ShapeDtypeStruct((LEV, ROWS, LANES), F32),
        ),
        in_specs=[member_block(LEV)] * count + [whole()] * (count + 1),
        out_specs=(pass_block(), whole()),
        compiler_params=pltpu.CompilerParams(dimension_semantics=ARB),
        cost_estimate=pl.CostEstimate(flops=400000000, bytes_accessed=9000000, transcendentals=0),
    )(*members, *fields, lat)


def merge_edges(left, right):
    inner = iota((ROWS, LANES), 1) & 31
    return jnp.where(inner < EDGE, left, right)


def columns_of_level(main, side, weights):
    high = jnp.concatenate([main[0], side[0]], axis=1)
    low = jnp.concatenate([main[1], side[1]], axis=1)
    return filter_columns(high, low, weights)


def single_of_level(main, side, weights):
    pad = jnp.zeros((ROWS, LANES), F32)
    main = halves(jnp.concatenate([main, pad], axis=0))
    side = halves(jnp.concatenate([side, pad], axis=0))
    return columns_of_level(main, side, weights)[:ROWS]


def side_fields(left_ref, right_ref, count, g):
    return [merge_edges(left_ref[x, g], right_ref[x, g]) for x in range(count)]


def middle_kernel(*refs):
    h_refs = refs[:5]
    main_ref, own_ref, static_ref, left_ref, right_ref, lat_ref, lon_ref, coef_ref, out_ref = refs[5:]
    lat = lat_ref[...]
    fields = [side_fields(left_ref, right_ref, 5, g) for g in range(2)]

    @pl.when(pl.program_id(0) == 0)
    def _():
        sides = [filter_single(fields[g], lat, 2) for g in range(2)]
        for l in range(LEV):
            single = single_of_level(static_ref[l], sides[l // 4], lon_ref[l % 4])
            out_ref[l] = coef_ref[1, l : l + 1, :] * single

    sides = [
        filter_rows(lambda k: [h[k, g].astype(F32) for h in h_refs], fields[g], lat, 2)
        for g in range(2)
    ]
    for l in range(LEV):
        value = columns_of_level((main_ref[0, l, 0], main_ref[0, l, 1]), sides[l // 4], lon_ref[l % 4])
        total = value[:ROWS] * own_ref[0, l].astype(F32)
        for k in range(1, STEP):
            total = total + value[8 * k : 8 * k + 8] * own_ref[k, l].astype(F32)
        out_ref[l] += coef_ref[0] * total


def middle(members, halos, passed, static, left, right, lat_mid, lon_mid, coefs):
    return pl.pallas_call(
        middle_kernel,
        grid=(MEM // STEP,),
        out_shape=jax.ShapeDtypeStruct((LEV, ROWS, LANES), F32),
        in_specs=[member_block(2)] * 5 + [pass_block(), member_block(LEV)] + [whole()] * 6,
        out_specs=whole(),
        compiler_params=pltpu.CompilerParams(dimension_semantics=ARB),
        cost_estimate=pl.CostEstimate(flops=400000000, bytes_accessed=9000000, transcendentals=0),
        name="middle",
    )(*halos, passed, members[2], static, left, right, lat_mid, lon_mid, coefs)


def final_kernel(*refs):
    h_refs = refs[:3]
    main_ref, static_ref, left_ref, right_ref, lat_ref, lon_ref, coef_ref, out_ref, single_ref = refs[3:]
    lat = lat_ref[...]
    fields = [side_fields(left_ref, right_ref, 3, g) for g in range(2)]
    scale = -HYBRID_ENSEMBLE / math.sqrt(MEM - 1)

    @pl.when(pl.program_id(0) == 0)
    def _():
        sides = [filter_single(fields[g], lat, 4) for g in range(2)]
        for l in range(LEV):
            single = single_of_level(static_ref[l], sides[l // 4], lon_ref[l % 4])
            single_ref[l] = coef_ref[2, l : l + 1, :] * single

    sides = [
        filter_rows(lambda k: [h[k, g].astype(F32) for h in h_refs], fields[g], lat, 4)
        for g in range(2)
    ]
    for l in range(LEV):
        value = columns_of_level((main_ref[0, l, 0], main_ref[0, l, 1]), sides[l // 4], lon_ref[l % 4])
        out_ref[:, l] = (scale * value).reshape(STEP, ROWS, LANES)


def final(halos, passed, static, left, right, lat_fin, lon_fin, coefs):
    return pl.pallas_call(
        final_kernel,
        grid=(MEM // STEP,),
        out_shape=(
            jax.ShapeDtypeStruct((MEM, LEV, ROWS, LANES), F32),
            jax.ShapeDtypeStruct((LEV, ROWS, LANES), F32),
        ),
        in_specs=[member_block(2)] * 3 + [pass_block()] + [whole()] * 6,
        out_specs=(member_block(LEV), whole()),
        compiler_params=pltpu.CompilerParams(dimension_semantics=ARB),
        cost_estimate=pl.CostEstimate(flops=400000000, bytes_accessed=9000000, transcendentals=0),
        name="final",
    )(*halos, passed, static, left, right, lat_fin, lon_fin, coefs)


def shift(value, axis, step):
    count = lax.axis_size(axis)
    return lax.ppermute(value, axis, [(i, (i + step) % count) for i in range(count)])


def edges_kernel(*refs):
    for x, ref in enumerate(refs[:-1]):
        refs[-1][x] = ref[LEV:]


def surround(forcing, reach):
    bands = range(reach, -reach - 1, -1)
    fields = [shift(forcing, "lat", d) if d else forcing for d in bands]
    edges = pl.pallas_call(
        edges_kernel,
        out_shape=jax.ShapeDtypeStruct((len(fields), 2, ROWS, LANES), F32),
        in_specs=[whole()] * len(fields),
        out_specs=whole(),
        cost_estimate=pl.CostEstimate(flops=100000, bytes_accessed=100000, transcendentals=0),
        name="edges",
    )(*near(*fields))
    return fields, shift(edges, "lon", 1), shift(edges, "lon", -1)


def route(buffer):
    buffer = buffer.reshape(DEV, 4, LANES)
    out = lax.all_to_all(buffer, ("lat", "lon"), split_axis=0, concat_axis=0, tiled=True)
    return out.reshape(BUF, LANES)


def per_device(
    ensemble,
    static_sigma,
    lat_taps,
    lon_taps,
    step_len,
    send_cols,
    send_count,
    obs_ref,
    obs_level,
    obs_weight,
    innovation,
    obs_precision,
):
    counts = jnp.broadcast_to(send_count.reshape(DEV, 1, 1), (DEV, 1, LANES))
    received = lax.all_to_all(counts, ("lat", "lon"), split_axis=0, concat_axis=0, tiled=True)
    received = received.reshape(DEV, LANES)
    level = obs_level.reshape(1, NOBS)
    ref = obs_ref.reshape(4, NOBS)
    weight = obs_weight.reshape(4, NOBS)
    innov = innovation.reshape(1, NOBS)
    precision = obs_precision.reshape(1, NOBS)

    band = lax.axis_index("lat").astype(I32).reshape(1)
    lat_mid, lon_mid, lat_fin, lon_fin, coefs, cells = matrices(
        band, lat_taps, lon_taps, static_sigma, step_len, send_cols.reshape(DEV, SLOT)
    )

    north = shift(ensemble, "lat", 1)
    south = shift(ensemble, "lat", -1)
    packed = pack(ensemble)
    from_left = shift(packed, "lon", 1)
    from_right = shift(packed, "lon", -1)
    north2 = shift(north, "lat", 1)
    south2 = shift(south, "lat", -1)
    members = [north2, north, ensemble, south, south2]

    outgoing, rows, lanes = first(received, ref, level, weight, precision, innov)
    outgoing, from_left, from_right = lax.optimization_barrier((outgoing, from_left, from_right))
    inner = lax.broadcasted_iota(I32, packed.shape, 3) & 31
    halo = jnp.where(inner < EDGE, from_left, from_right)
    halos = [shift(halo, "lat", d) if d else halo for d in (2, 1, 0, -1, -2)]

    arrived = route(outgoing)
    forcing = columns(arrived, cells)
    fields, left, right = surround(forcing, 2)
    passed, static = filtered(members, fields, lat_mid, 2)
    increment = middle(members, halos, passed, static, left, right, lat_mid, lon_mid, coefs)
    incoming = route(slots(increment.reshape(LEV * ROWS, LANES), cells))
    outgoing, departure = second(incoming, rows, lanes, weight, precision, innov, coefs)
    fields, left, right = surround(columns(route(outgoing), cells), 1)
    passed, static = filtered(members[1:4], fields, lat_fin, 4)
    control, static = final(halos[1:4], passed, static, left, right, lat_fin, lon_fin, coefs)
    return (control, static, departure.reshape(1, 1, -1))


def solution(mesh):
    return jax.shard_map(
        per_device,
        mesh=mesh,
        in_specs=(
            P(None, None, "lat", "lon"),
            P(),
            P(),
            P(),
            P(),
            P("lat", "lon", None, None),
            P("lat", "lon", None),
            P("lat", "lon", None, None),
            P("lat", "lon", None),
            P("lat", "lon", None, None),
            P("lat", "lon", None),
            P("lat", "lon", None),
        ),
        out_specs=(P(None, None, "lat", "lon"), P(None, "lat", "lon"), P("lat", "lon", None)),
        check_vma=False,
    )
```

```python
import functools
import math

import jax
import jax.numpy as jnp
from jax import lax
from jax.experimental import pallas as pl
from jax.experimental.pallas import tpu as pltpu
from jax.sharding import PartitionSpec as P


HYBRID_STATIC = 0.5
HYBRID_ENSEMBLE = 0.8660254037844386
F32 = jnp.float32
BF16 = jnp.bfloat16
I32 = jnp.int32

MEM = 80
LEV = 8
ROWS = 8
LANES = 128
NOBS = 2048
SLOT = 64
DEV = 128
NLAT = 64
HW = 8
TAPS = 17
EDGE = 16
BUF = DEV * 4
PAIRS = DEV // 2

VMEM = pltpu.VMEM
ARB = ("arbitrary",)
LIMIT = 20 * 2**20


def whole(memory_space=VMEM):
    return pl.BlockSpec(memory_space=memory_space)


def placed(space, *arrays):
    return [pltpu.with_memory_space_constraint(a, space) for a in arrays]


def near(*arrays):
    return placed(VMEM, *arrays)


def split(value):
    high = value.astype(BF16).astype(F32)
    return high, value - high


def iota(shape, dim):
    return lax.broadcasted_iota(I32, shape, dim)


def nn(a, b):
    return lax.dot_general(a, b, (((1,), (0,)), ((), ())), preferred_element_type=F32)


def nt(a, b):
    return lax.dot_general(a, b, (((1,), (1,)), ((), ())), preferred_element_type=F32)


def matrices_kernel(
    band_ref, lat_ref, lon_ref, sigma_ref, step_ref, cols_ref,
    lat_mid, lon_mid, lat_fin, lon_fin, coef_ref, cell_ref,
):
    base = band_ref[0] * ROWS
    cell_ref[...] = jnp.concatenate(
        [cols_ref[pl.ds(h, PAIRS, stride=2), :] for h in range(2)], axis=1
    )
    ens_scale = HYBRID_ENSEMBLE / math.sqrt(MEM - 1)
    level = iota((LEV, LANES), 0)
    sigma = jnp.zeros((LEV, LANES), F32)
    for l in range(LEV):
        sigma = jnp.where(level == l, sigma_ref[l], sigma)
    once = jnp.ones((LEV, LANES), F32)
    step0 = once * step_ref[0]
    step1 = once * step_ref[1]
    coef_ref[0] = step0 * (-ens_scale * ens_scale)
    coef_ref[1] = step0 * sigma * sigma * (-HYBRID_STATIC * HYBRID_STATIC)
    coef_ref[2] = sigma * -HYBRID_STATIC
    coef_ref[3] = (1.0 - step1) * step0
    coef_ref[4] = step1

    def pick(index, taps):
        out = jnp.zeros(index.shape, F32)
        for t in range(TAPS):
            out = jnp.where(index == t, taps[t], out)
        return out

    row = iota((8, 160), 0)
    col = iota((8, 160), 1)
    group = sum((col >= 40 * n).astype(I32) for n in range(1, 4))
    offset = col - 40 * group
    diff = row - offset + 2 * HW
    source = base - 2 * HW + offset
    total = jnp.zeros((8, 160), F32)
    for t in range(TAPS):
        middle = base + row + t - HW
        valid = jnp.logical_and(middle >= 0, middle < NLAT)
        total = total + jnp.where(valid, lat_ref[t] * pick(diff + t, lat_ref), 0.0)
    total = jnp.where(jnp.logical_and(source >= 0, source < NLAT), total, 0.0)
    high, low = split(total)
    blocks = []
    for s in range(2):
        blocks.append(jnp.where((group & 1) == s, high, 0.0))
        blocks.append(jnp.where(group == s, low, 0.0))
    lat_mid[...] = jnp.concatenate(blocks, axis=0).astype(BF16)

    row = iota((8, 192), 0)
    col = iota((8, 192), 1)
    group = sum((col >= 24 * n).astype(I32) for n in range(1, 8))
    offset = col - 24 * group
    source = base - HW + offset
    total = pick(row - offset + 2 * HW, lat_ref)
    total = jnp.where(jnp.logical_and(source >= 0, source < NLAT), total, 0.0)
    high, low = split(total)
    blocks = []
    for s in range(4):
        blocks.append(jnp.where((group & 3) == s, high, 0.0))
        blocks.append(jnp.where(group == s, low, 0.0))
    lat_fin[...] = jnp.concatenate(blocks, axis=0).astype(BF16)

    lag = iota((8, LANES), 1) - 2 * HW
    auto = jnp.zeros((8, LANES), F32)
    for t in range(TAPS):
        auto = auto + lon_ref[t] * pick(lag + t, lon_ref)

    def auto_at(n):
        return jnp.sum(jnp.where(lag[:1] == n, auto[:1], 0.0), axis=1, keepdims=True)

    coefficients = [auto_at(n) for n in range(2 * HW + 1)]
    main = iota((LANES, LANES), 0) - iota((LANES, LANES), 1)
    edge = iota((32, LANES), 0)
    edge = jnp.where(edge < EDGE, edge - EDGE, edge + LANES - EDGE) - iota((32, LANES), 1)

    def smooth_twice(distance):
        distance = jnp.abs(distance)
        out = jnp.zeros(distance.shape, F32)
        for n in range(2 * HW + 1):
            out = jnp.where(distance == n, coefficients[n], out)
        return out

    def place(out_ref, main_value, edge_value):
        main_high, main_low = split(main_value)
        edge_high, edge_low = split(edge_value)
        for v in range(4):
            out_ref[v, :LANES, :LANES] = main_high.astype(BF16)
            out_ref[v, :LANES, LANES:] = main_low.astype(BF16)
            out_ref[v, LANES:, :] = jnp.zeros((LANES, 2 * LANES), BF16)
            out_ref[v, LANES + 32 * v : LANES + 32 * (v + 1), :LANES] = edge_high.astype(BF16)
            out_ref[v, LANES + 32 * v : LANES + 32 * (v + 1), LANES:] = edge_low.astype(BF16)

    place(lon_mid, smooth_twice(main), smooth_twice(edge))
    place(lon_fin, pick(HW - main, lon_ref), pick(HW - edge, lon_ref))


def matrices(band, lat_taps, lon_taps, static_sigma, step_len, cols):
    smem = whole(pltpu.SMEM)
    return pl.pallas_call(
        matrices_kernel,
        out_shape=(
            VMEM((32, 160), BF16),
            VMEM((4, 256, 256), BF16),
            VMEM((64, 192), BF16),
            VMEM((4, 256, 256), BF16),
            VMEM((5, LEV, LANES), F32),
            VMEM((PAIRS, LANES), I32),
        ),
        in_specs=[smem] * 5 + [whole()],
        out_specs=(whole(),) * 6,
        compiler_params=pltpu.CompilerParams(vmem_limit_bytes=LIMIT),
        cost_estimate=pl.CostEstimate(flops=4000000, bytes_accessed=1100000, transcendentals=0),
        name="matrices",
    )(band, *placed(pltpu.HBM, lat_taps, lon_taps, static_sigma, step_len), cols)


def pack_kernel(e_ref, out_ref):
    row = iota((LANES, LANES), 0)
    col = iota((LANES, LANES), 1)
    inner = col & 31
    source = jnp.where(inner < EDGE, inner + LANES - EDGE, inner - EDGE)
    count = e_ref.shape[0]
    chooses = []
    for v in range(4):
        choose = jnp.logical_and(row == source, (col >> 5) == v)
        chooses.append(jnp.where(choose, 1.0, 0.0).astype(BF16))
    choose = [jnp.concatenate(chooses[2 * h : 2 * h + 2], axis=0) for h in range(2)]
    for g in range(2):
        total = None
        for h in range(2):
            tiles = [
                e_ref[:, 4 * g + 2 * h + v].astype(F32).reshape(count * ROWS, LANES).astype(BF16)
                for v in range(2)
            ]
            part = nn(jnp.concatenate(tiles, axis=1), choose[h])
            total = part if total is None else total + part
        out_ref[:, g] = total.reshape(count, ROWS, LANES).astype(BF16)


def pack(ensemble):
    step = 16
    return pl.pallas_call(
        pack_kernel,
        grid=(MEM // step,),
        out_shape=jax.ShapeDtypeStruct((MEM, 2, ROWS, LANES), BF16),
        in_specs=[pl.BlockSpec((step, LEV, ROWS, LANES), lambda i: (i, 0, 0, 0))],
        out_specs=pl.BlockSpec((step, 2, ROWS, LANES), lambda i: (i, 0, 0, 0)),
        compiler_params=pltpu.CompilerParams(dimension_semantics=ARB, vmem_limit_bytes=LIMIT),
        cost_estimate=pl.CostEstimate(flops=4000000, bytes_accessed=1600000, transcendentals=0),
        name="pack",
    )(ensemble)


CHUNK = 256
UNROLL = 2


def place_values(acc_ref, row_hot, lane_of, value_of, lane_iota):
    parts_high, parts_low = [], []
    for q in range(4):
        hit = lane_iota == lane_of[q]
        high, low = split(value_of[q])
        parts_high.append(jnp.where(hit, high, 0.0).astype(BF16))
        parts_low.append(jnp.where(hit, low, 0.0).astype(BF16))
    values = jnp.concatenate(
        [jnp.concatenate(parts_high, axis=1), jnp.concatenate(parts_low, axis=1)], axis=0
    )
    acc_ref[...] += nt(row_hot, values)


def hot_rows(row_of, row_iota):
    parts = [jnp.where(row_iota == row_of[q], 1.0, 0.0).astype(BF16) for q in range(4)]
    return jnp.concatenate(parts, axis=1)


def first_kernel(
    count_ref, ref_ref, level_ref, weight_ref, precision_ref, innovation_ref,
    buffer_ref, row_ref, lane_ref, acc_ref,
):
    counts = count_ref[...].astype(F32)
    below = iota((DEV, DEV), 1) <= iota((DEV, DEV), 0)
    ends = nn(jnp.where(below, 1.0, 0.0).astype(BF16), counts.astype(BF16))
    counts = jnp.concatenate([counts] * (CHUNK // LANES), axis=1)
    ends = jnp.concatenate([ends] * (CHUNK // LANES), axis=1)
    acc_ref[...] = jnp.zeros_like(acc_ref)
    row_iota = iota((BUF, CHUNK), 0).astype(F32)
    lane_iota = iota((LANES, CHUNK), 0).astype(F32)

    @pl.loop(0, NOBS // CHUNK, unroll=UNROLL)
    def _(c):
        part = pl.ds(pl.multiple_of(c * CHUNK, CHUNK), CHUNK)
        level = level_ref[:, part]
        low_level = (level & 3).astype(F32)
        high_level = ((level >> 2) * SLOT).astype(F32)
        forced = -(precision_ref[:, part] * innovation_ref[:, part])
        rows, lanes, values = [], [], []
        for q in range(4):
            position = ref_ref[q : q + 1, part].astype(F32)
            passed = position >= ends
            source = jnp.sum(jnp.where(passed, 1.0, 0.0), axis=0, keepdims=True)
            start = jnp.sum(jnp.where(passed, counts, 0.0), axis=0, keepdims=True)
            rows.append(source * 4.0 + low_level)
            lanes.append(high_level + position - start)
            row_ref[q : q + 1, part] = rows[q]
            lane_ref[q : q + 1, part] = lanes[q]
            values.append(weight_ref[q : q + 1, part] * forced)
        place_values(acc_ref, hot_rows(rows, row_iota), lanes, values, lane_iota)

    buffer_ref[...] = acc_ref[:, :LANES] + acc_ref[:, LANES:]


def first(count, ref, level, weight, precision, innovation):
    return pl.pallas_call(
        first_kernel,
        out_shape=(
            jax.ShapeDtypeStruct((BUF, LANES), F32),
            VMEM((4, NOBS), F32),
            VMEM((4, NOBS), F32),
        ),
        in_specs=[whole()] * 6,
        out_specs=(whole(),) * 3,
        scratch_shapes=[VMEM((BUF, 2 * LANES), F32)],
        compiler_params=pltpu.CompilerParams(vmem_limit_bytes=LIMIT),
        cost_estimate=pl.CostEstimate(flops=40000000, bytes_accessed=600000, transcendentals=0),
        name="first",
    )(*near(count), ref, level, weight, precision, innovation)


def second_kernel(
    incoming_ref, row_ref, lane_ref, weight_ref, precision_ref, innovation_ref, coef_ref,
    buffer_ref, departure_ref, acc_ref,
):
    flipped = incoming_ref[...].T
    high, low = split(flipped)
    table = jnp.concatenate([high, low], axis=0).astype(BF16)
    acc_ref[...] = jnp.zeros_like(acc_ref)
    row_iota = iota((BUF, CHUNK), 0).astype(F32)
    lane_iota = iota((LANES, CHUNK), 0).astype(F32)
    earlier = coef_ref[3, :1, :1]
    later = coef_ref[4, :1, :1]

    @pl.loop(0, NOBS // CHUNK, unroll=1)
    def _(c):
        part = pl.ds(pl.multiple_of(c * CHUNK, CHUNK), CHUNK)
        rows = [row_ref[q : q + 1, part] for q in range(4)]
        lanes = [lane_ref[q : q + 1, part] for q in range(4)]
        weights = [weight_ref[q : q + 1, part] for q in range(4)]
        innovation = innovation_ref[:, part]
        row_hot = hot_rows(rows, row_iota)
        found = nn(table, row_hot)
        found = found[:LANES] + found[LANES:]
        departure = -innovation
        for q in range(4):
            column = found[:, q * CHUNK : (q + 1) * CHUNK]
            picked = jnp.sum(jnp.where(lane_iota == lanes[q], column, 0.0), axis=0, keepdims=True)
            departure = departure + weights[q] * picked
        departure_ref[:, part] = departure
        forced = precision_ref[:, part] * (later * departure - earlier * innovation)
        values = [weights[q] * forced for q in range(4)]
        place_values(acc_ref, row_hot, lanes, values, lane_iota)

    buffer_ref[...] = acc_ref[:, :LANES] + acc_ref[:, LANES:]


def second(incoming, rows, lanes, weight, precision, innovation, coefs):
    return pl.pallas_call(
        second_kernel,
        out_shape=(
            jax.ShapeDtypeStruct((BUF, LANES), F32),
            jax.ShapeDtypeStruct((1, NOBS), F32),
        ),
        in_specs=[whole()] * 7,
        out_specs=(whole(),) * 2,
        scratch_shapes=[VMEM((BUF, 2 * LANES), F32)],
        compiler_params=pltpu.CompilerParams(vmem_limit_bytes=LIMIT),
        cost_estimate=pl.CostEstimate(flops=60000000, bytes_accessed=800000, transcendentals=0),
        name="second",
    )(*near(incoming), rows, lanes, weight, precision, innovation, coefs)


def swap_quadrants(tile):
    sub = iota((8, LANES), 0) < 4
    lane = iota((8, LANES), 1) < SLOT
    moved = pltpu.roll(pltpu.roll(tile, 4, 0), SLOT, 1)
    return jnp.where(sub == lane, tile, moved)


GROUP = 4


def columns_kernel(buffer_ref, cell_ref, out_ref, grid_ref):
    lane_iota = iota((LANES, LANES), 0)
    total = jnp.zeros((LANES, LANES), F32)
    for n in range(0, PAIRS, GROUP):
        values, hots = [], []
        for m in range(n, n + GROUP):
            tile = swap_quadrants(buffer_ref[8 * m : 8 * m + 8, :])
            cell = cell_ref[m : m + 1, :]
            row = cell >> 7
            high, low = split(tile)
            masks = [row == r for r in range(ROWS)]
            values.append(
                jnp.concatenate(
                    [jnp.where(k, high, 0.0) for k in masks] + [jnp.where(k, low, 0.0) for k in masks],
                    axis=0,
                ).astype(BF16)
            )
            hots.append(jnp.where(lane_iota == (cell & 127), 1.0, 0.0).astype(BF16))
        total = total + nt(jnp.concatenate(values, axis=1), jnp.concatenate(hots, axis=1))

    grid_ref[...] = total[:64] + total[64:]
    lane = iota((ROWS, LANES), 1)
    inner = lane & 31
    edges = [jnp.zeros((ROWS, LANES), F32)] * 2
    for l in range(LEV):
        tile = grid_ref[pl.ds(l, ROWS, stride=LEV), :]
        out_ref[l] = tile
        v = l % 4
        right = pltpu.roll(tile, (32 * v + EDGE) % LANES, 1)
        left = pltpu.roll(tile, (32 * v + EDGE) % LANES, 1)
        moved = jnp.where(inner < EDGE, right, left)
        edges[l // 4] = jnp.where((lane >> 5) == v, moved, edges[l // 4])
    out_ref[LEV] = edges[0]
    out_ref[LEV + 1] = edges[1]


def columns(buffer, cells):
    return pl.pallas_call(
        columns_kernel,
        out_shape=VMEM((LEV + 2, ROWS, LANES), F32),
        in_specs=[whole()] * 2,
        out_specs=whole(),
        scratch_shapes=[VMEM((64, LANES), F32)],
        compiler_params=pltpu.CompilerParams(vmem_limit_bytes=LIMIT),
        cost_estimate=pl.CostEstimate(flops=20000000, bytes_accessed=400000, transcendentals=0),
        name="columns",
    )(*near(buffer), cells)


def slots_kernel(increment_ref, cell_ref, out_ref):
    rows = [increment_ref[pl.ds(r, LEV, stride=ROWS), :] for r in range(ROWS)]
    pairs = [split(value) for value in rows]
    table = jnp.concatenate([p[0] for p in pairs] + [p[1] for p in pairs], axis=0).astype(BF16)
    lane_iota = iota((LANES, LANES), 0)

    for n in range(0, PAIRS, GROUP):
        hots, cells = [], []
        for m in range(n, n + GROUP):
            cell = cell_ref[m : m + 1, :]
            cells.append(cell >> 7)
            hots.append(jnp.where(lane_iota == (cell & 127), 1.0, 0.0).astype(BF16))
        found = nn(table, jnp.concatenate(hots, axis=1))
        found = found[:64] + found[64:]
        for g in range(GROUP):
            tile = jnp.zeros((LEV, LANES), F32)
            for r in range(ROWS):
                part = found[8 * r : 8 * r + 8, g * LANES : (g + 1) * LANES]
                tile = jnp.where(cells[g] == r, part, tile)
            out_ref[8 * (n + g) : 8 * (n + g) + 8, :] = swap_quadrants(tile)


def slots(increment, cells):
    return pl.pallas_call(
        slots_kernel,
        out_shape=jax.ShapeDtypeStruct((BUF, LANES), F32),
        in_specs=[whole()] * 2,
        out_specs=whole(),
        compiler_params=pltpu.CompilerParams(vmem_limit_bytes=LIMIT),
        cost_estimate=pl.CostEstimate(flops=20000000, bytes_accessed=400000, transcendentals=0),
        name="slots",
    )(*near(increment), cells)


STEP = 16


def column_of(tiles):
    value = jnp.concatenate(tiles, axis=0)
    high = value.astype(BF16)
    low = (value - high.astype(F32)).astype(BF16)
    return jnp.concatenate([high, low], axis=0)


def halves(value):
    high = value.astype(BF16)
    return high, (value - high.astype(F32)).astype(BF16)


def block(value, s, n):
    tile = value[16 * s : 16 * s + 16, n * LANES : (n + 1) * LANES]
    return tile[:8] + tile[8:]


def filter_rows(tiles_of, fields, lat, stack):
    per = STEP // stack
    out = [None] * STEP
    for c in range(0, per, 2):
        parts = []
        for n in range(c, c + 2):
            tiles = []
            for s in range(stack):
                tiles += [t * f for t, f in zip(tiles_of(s * per + n), fields)]
            parts.append(column_of(tiles))
        value = nn(lat, jnp.concatenate(parts, axis=1))
        for s in range(stack):
            for n in range(2):
                out[s * per + c + n] = block(value, s, n)
    return halves(jnp.concatenate(out, axis=0))


def filter_single(fields, lat, stack):
    blank = [jnp.zeros((ROWS, LANES), F32)] * (len(fields) * (stack - 1))
    return block(nn(lat, column_of(list(fields) + blank)), 0, 0)


def filter_columns(high, low, weights):
    value = nn(high, weights) + nn(low, weights)
    return value[:, :LANES] + value[:, LANES:]


def rows_kernel(count, stack, *refs):
    e_refs = refs[:count]
    f_refs = refs[count : 2 * count]
    lat_ref, out_ref, static_ref = refs[2 * count :]
    lat = lat_ref[...]
    step = pl.program_id(0)
    base = step * STEP

    @pl.when(pl.program_id(0) == 0)
    def _():
        for l in range(LEV):
            static_ref[l] = filter_single([f[l] for f in f_refs], lat, stack)

    for l in range(LEV):
        high, low = filter_rows(
            lambda k: [e[base + k, l].astype(F32) for e in e_refs], [f[l] for f in f_refs], lat, stack
        )
        out_ref[step, l, 0] = high
        out_ref[step, l, 1] = low


def member_block(depth):
    return pl.BlockSpec((STEP, depth, ROWS, LANES), lambda i: (i, 0, 0, 0))


def filtered(members, fields, lat, stack):
    count = len(members)
    return pl.pallas_call(
        functools.partial(rows_kernel, count, stack),
        grid=(MEM // STEP,),
        out_shape=(
            VMEM((MEM // STEP, LEV, 2, STEP * ROWS, LANES), BF16),
            VMEM((LEV, ROWS, LANES), F32),
        ),
        in_specs=[whole()] * (2 * count + 1),
        out_specs=(whole(), whole()),
        compiler_params=pltpu.CompilerParams(dimension_semantics=ARB, vmem_limit_bytes=LIMIT),
        cost_estimate=pl.CostEstimate(flops=400000000, bytes_accessed=9000000, transcendentals=0),
    )(*near(*members, *fields), lat)


def merge_edges(left, right):
    inner = iota((ROWS, LANES), 1) & 31
    return jnp.where(inner < EDGE, left, right)


def columns_of_level(main, side, weights):
    high = jnp.concatenate([main[0], side[0]], axis=1)
    low = jnp.concatenate([main[1], side[1]], axis=1)
    return filter_columns(high, low, weights)


def single_of_level(main, side, weights):
    pad = jnp.zeros((ROWS, LANES), F32)
    main = halves(jnp.concatenate([main, pad], axis=0))
    side = halves(jnp.concatenate([side, pad], axis=0))
    return columns_of_level(main, side, weights)[:ROWS]


def side_fields(left_ref, right_ref, count, g):
    return [merge_edges(left_ref[x, g], right_ref[x, g]) for x in range(count)]


def middle_kernel(*refs):
    h_refs = refs[:5]
    main_ref, own_ref, static_ref, left_ref, right_ref, lat_ref, lon_ref, coef_ref, out_ref = refs[5:]
    lat = lat_ref[...]
    fields = [side_fields(left_ref, right_ref, 5, g) for g in range(2)]
    step = pl.program_id(0)
    base = step * STEP

    @pl.when(pl.program_id(0) == 0)
    def _():
        sides = [filter_single(fields[g], lat, 2) for g in range(2)]
        for l in range(LEV):
            single = single_of_level(static_ref[l], sides[l // 4], lon_ref[l % 4])
            out_ref[l] = coef_ref[1, l : l + 1, :] * single

    sides = [
        filter_rows(lambda k: [h[base + k, g].astype(F32) for h in h_refs], fields[g], lat, 2)
        for g in range(2)
    ]
    for l in range(LEV):
        value = columns_of_level((main_ref[step, l, 0], main_ref[step, l, 1]), sides[l // 4], lon_ref[l % 4])
        total = value[:ROWS] * own_ref[base, l].astype(F32)
        for k in range(1, STEP):
            total = total + value[8 * k : 8 * k + 8] * own_ref[base + k, l].astype(F32)
        out_ref[l] += coef_ref[0] * total


def middle(members, halos, passed, static, left, right, lat_mid, lon_mid, coefs):
    return pl.pallas_call(
        middle_kernel,
        grid=(MEM // STEP,),
        out_shape=VMEM((LEV, ROWS, LANES), F32),
        in_specs=[whole()] * 13,
        out_specs=whole(),
        compiler_params=pltpu.CompilerParams(dimension_semantics=ARB, vmem_limit_bytes=LIMIT),
        cost_estimate=pl.CostEstimate(flops=400000000, bytes_accessed=9000000, transcendentals=0),
        name="middle",
    )(*near(*halos, passed, members[2], static, left, right), lat_mid, lon_mid, coefs)


def final_kernel(*refs):
    h_refs = refs[:3]
    main_ref, static_ref, left_ref, right_ref, lat_ref, lon_ref, coef_ref, out_ref, single_ref = refs[3:]
    lat = lat_ref[...]
    fields = [side_fields(left_ref, right_ref, 3, g) for g in range(2)]
    step = pl.program_id(0)
    base = step * STEP
    scale = -HYBRID_ENSEMBLE / math.sqrt(MEM - 1)

    @pl.when(pl.program_id(0) == 0)
    def _():
        sides = [filter_single(fields[g], lat, 4) for g in range(2)]
        for l in range(LEV):
            single = single_of_level(static_ref[l], sides[l // 4], lon_ref[l % 4])
            single_ref[l] = coef_ref[2, l : l + 1, :] * single

    sides = [
        filter_rows(lambda k: [h[base + k, g].astype(F32) for h in h_refs], fields[g], lat, 4)
        for g in range(2)
    ]
    for l in range(LEV):
        value = columns_of_level((main_ref[step, l, 0], main_ref[step, l, 1]), sides[l // 4], lon_ref[l % 4])
        out_ref[:, l] = (scale * value).reshape(STEP, ROWS, LANES)


def final(halos, passed, static, left, right, lat_fin, lon_fin, coefs):
    return pl.pallas_call(
        final_kernel,
        grid=(MEM // STEP,),
        out_shape=(
            jax.ShapeDtypeStruct((MEM, LEV, ROWS, LANES), F32),
            jax.ShapeDtypeStruct((LEV, ROWS, LANES), F32),
        ),
        in_specs=[whole()] * 10,
        out_specs=(member_block(LEV), whole()),
        compiler_params=pltpu.CompilerParams(dimension_semantics=ARB, vmem_limit_bytes=LIMIT),
        cost_estimate=pl.CostEstimate(flops=400000000, bytes_accessed=9000000, transcendentals=0),
        name="final",
    )(*near(*halos, passed, static, left, right), lat_fin, lon_fin, coefs)


def shift(value, axis, step):
    count = lax.axis_size(axis)
    return lax.ppermute(value, axis, [(i, (i + step) % count) for i in range(count)])


def edges_kernel(*refs):
    for x, ref in enumerate(refs[:-1]):
        refs[-1][x] = ref[LEV:]


def surround(forcing, reach):
    bands = range(reach, -reach - 1, -1)
    fields = [shift(forcing, "lat", d) if d else forcing for d in bands]
    edges = pl.pallas_call(
        edges_kernel,
        out_shape=VMEM((len(fields), 2, ROWS, LANES), F32),
        in_specs=[whole()] * len(fields),
        out_specs=whole(),
        compiler_params=pltpu.CompilerParams(vmem_limit_bytes=LIMIT),
        cost_estimate=pl.CostEstimate(flops=100000, bytes_accessed=100000, transcendentals=0),
        name="edges",
    )(*near(*fields))
    return fields, shift(edges, "lon", 1), shift(edges, "lon", -1)


def route(buffer):
    buffer = buffer.reshape(DEV, 4, LANES)
    out = lax.all_to_all(buffer, ("lat", "lon"), split_axis=0, concat_axis=0, tiled=True)
    return out.reshape(BUF, LANES)


def per_device(
    ensemble,
    static_sigma,
    lat_taps,
    lon_taps,
    step_len,
    send_cols,
    send_count,
    obs_ref,
    obs_level,
    obs_weight,
    innovation,
    obs_precision,
):
    counts = jnp.broadcast_to(send_count.reshape(DEV, 1, 1), (DEV, 1, LANES))
    received = lax.all_to_all(counts, ("lat", "lon"), split_axis=0, concat_axis=0, tiled=True)
    received = received.reshape(DEV, LANES)
    level = obs_level.reshape(1, NOBS)
    ref = obs_ref.reshape(4, NOBS)
    weight = obs_weight.reshape(4, NOBS)
    innov = innovation.reshape(1, NOBS)
    precision = obs_precision.reshape(1, NOBS)

    band = lax.axis_index("lat").astype(I32).reshape(1)
    lat_mid, lon_mid, lat_fin, lon_fin, coefs, cells = matrices(
        band, lat_taps, lon_taps, static_sigma, step_len, send_cols.reshape(DEV, SLOT)
    )

    north = shift(ensemble, "lat", 1)
    south = shift(ensemble, "lat", -1)
    packed = pack(ensemble)
    from_left = shift(packed, "lon", 1)
    from_right = shift(packed, "lon", -1)
    north2 = shift(north, "lat", 1)
    south2 = shift(south, "lat", -1)
    members = [north2, north, ensemble, south, south2]

    outgoing, rows, lanes = first(received, ref, level, weight, precision, innov)
    outgoing, from_left, from_right = lax.optimization_barrier((outgoing, from_left, from_right))
    inner = lax.broadcasted_iota(I32, packed.shape, 3) & 31
    halo = jnp.where(inner < EDGE, from_left, from_right)
    halos = [shift(halo, "lat", d) if d else halo for d in (2, 1, 0, -1, -2)]

    arrived = route(outgoing)
    forcing = columns(arrived, cells)
    fields, left, right = surround(forcing, 2)
    passed, static = filtered(members, fields, lat_mid, 2)
    increment = middle(members, halos, passed, static, left, right, lat_mid, lon_mid, coefs)
    incoming = route(slots(increment.reshape(LEV * ROWS, LANES), cells))
    outgoing, departure = second(incoming, rows, lanes, weight, precision, innov, coefs)
    fields, left, right = surround(columns(route(outgoing), cells), 1)
    passed, static = filtered(members[1:4], fields, lat_fin, 4)
    control, static = final(halos[1:4], passed, static, left, right, lat_fin, lon_fin, coefs)
    return (control, static, departure.reshape(1, 1, -1))


def solution(mesh):
    return jax.shard_map(
        per_device,
        mesh=mesh,
        in_specs=(
            P(None, None, "lat", "lon"),
            P(),
            P(),
            P(),
            P(),
            P("lat", "lon", None, None),
            P("lat", "lon", None),
            P("lat", "lon", None, None),
            P("lat", "lon", None),
            P("lat", "lon", None, None),
            P("lat", "lon", None),
            P("lat", "lon", None),
        ),
        out_specs=(P(None, None, "lat", "lon"), P(None, "lat", "lon"), P("lat", "lon", None)),
        check_vma=False,
    )
```
